32 devices in a mesh: slab: 8 (over z, x), gy: 4 (over y, core).
Axes of the slice: x: 2, y: 2, z: 4, core: 2. Of those that a mesh axis runs over, the one named last changes fastest.
Arguments:
- displacement: float32 [3, 32, 64, 512], P(None, None, 'slab', 'gy'), may hold values from -6 to 6
- previous: float32 [3, 32, 64, 512], P(None, None, 'slab', 'gy'), may hold values from -6 to 6
- shear_coef: float32 [32, 64, 512], P(None, 'slab', 'gy'), may hold values from 0.04 to 0.16
- bulk_coef: float32 [32, 64, 512], P(None, 'slab', 'gy'), may hold values from 0.02 to 0.16
- cell_index: int32 [32768], P(('slab', 'gy')), may hold values from 0 to 32767, as said below
- archetype_id: int32 [32768, 1], P(('slab', 'gy')), may hold values from 0 to 1023; in each aligned block of 1024 rows (0 to 1023, 1024 to 2047, ...) at most 2 rows name the same one
- transition: bfloat16 [1024, 256, 256], P(('slab', 'gy')), may hold values from -1 to 1
- forcing: float32 [1024, 3, 256], P(('slab', 'gy')), may hold values from -3 to 3
Outputs:
- final_field: float32 [3, 32, 64, 512], P(None, None, 'slab', 'gy')
- building_state: float32 [32768, 256], P(('slab', 'gy'))
The draws below stay inside these ranges and needn't reach their ends.
Inputs may be any that keep to these rules, and one draw needn't show every extreme that they name: `cell_index`: building b's cell has x between s * 8 and s * 8 + 7, where s = (b // 1024) // 4; y is any. `archetype_id`: among the 1024 buildings of one device no archetype appears more than 2 times.
All inputs are finite; a program needn't handle non-finite values.
Results may differ from the reference program's by a relative error of at most 0.0023.
Values sent between devices are 32-bit elements; how exact they have to be, the bound alone decides.
A program may use at most 64 MiB of HBM per device.

```python
import math
import jax
import jax.numpy as jnp
import numpy as np
from jax import lax

NZ = 32
CX = 8
CY = 128
ARCHETYPES = 1024
STATES = 256
BLD_DEV = 1024
COUPLINGS = 4
EVERY = 5
SUB = 6
NX = 64
NY = 512
BUILDINGS = 32768
CAP = 2
DEVICES = 32


def draw_cell_index(key, part):
    rows = jnp.arange(BUILDINGS, dtype=jnp.int32)
    strip = rows // BLD_DEV // (NY // CY)
    key_x, key_y = jax.random.split(jax.random.fold_in(key, 11))
    along_x = jax.random.randint(key_x, (BUILDINGS,), 0, CX, dtype=jnp.int32)
    along_y = jax.random.randint(key_y, (BUILDINGS,), 0, NY, dtype=jnp.int32)
    return ((strip * CX + along_x) * NY + along_y).astype(jnp.int32)


def draw_transition(key, part):
    key_a, key_b = jax.random.split(jax.random.fold_in(key, 7))
    noise = jax.random.normal(key_a, (ARCHETYPES, STATES, STATES), jnp.float32) * (0.2 / math.sqrt(STATES))
    noise = jnp.clip(noise, -0.25, 0.25)
    diagonal = jax.random.uniform(key_b, (ARCHETYPES, STATES), jnp.float32, 0.4, 0.7)
    matrix = noise + diagonal[:, :, None] * jnp.eye(STATES, dtype=jnp.float32)[None]
    return matrix.astype(jnp.bfloat16)


def block_levels(own_key, dims, cuts, smallest, high):
    def one(dim, blocks):
        heights = jax.random.uniform(jax.random.fold_in(jax.random.fold_in(own_key, 6), dim), (blocks,), jnp.float32, smallest / len(cuts), high / len(cuts))
        return jnp.repeat(jnp.exp(heights), dims[dim] // blocks).reshape((-1,) + (1,) * (len(dims) - dim - 1))

    factor_of = one(*cuts[0])
    for cut in cuts[1:]:
        factor_of = factor_of * one(*cut)
    return factor_of


def deal_out(stream_key, own, number, rows, number_of, top, bound, lean):
    sequence = jax.random.permutation(stream_key, number_of)
    crowded, ordinary = load_shares(number_of, rows * top, bound, lean, True), load_shares(number_of, rows * top, bound, lean, False)
    places = jnp.arange(number_of)

    def named(tallies, rotation):
        used = int((tallies > 0).sum())
        fixed = max(1, used // 4)
        moved = fixed + (places - fixed + rotation * (used - fixed)) % max(1, number_of - fixed)
        return jnp.zeros((number_of,), jnp.int32).at[sequence[jnp.where(places < fixed, places, moved)]].set(jnp.asarray(tallies, jnp.int32))

    tallies = jnp.where(number % 4 == 0, named(crowded, number // 4), named(ordinary, number - number // 4 - 1))
    mixed = jax.random.permutation(jax.random.fold_in(own, 3), number_of)
    giver, sink = mixed[0:number_of // 2 * 2:2], mixed[1:number_of // 2 * 2:2]
    room = jnp.minimum(tallies[giver] - 1, bound - tallies[sink]) // 2
    room = jnp.where((giver == sequence[0]) | (sink == sequence[0]) | (tallies[sink] == 0), 0, jnp.maximum(room, 0))
    moved = jax.random.randint(jax.random.fold_in(own, 4), (number_of // 2,), 0, 1 << 20) % (room + 1)
    tallies = tallies.at[giver].add(-moved).at[sink].add(moved)
    items = jnp.searchsorted(jnp.cumsum(tallies), jnp.arange(rows * top), side="right").astype(jnp.int32)
    table = items.reshape(top, rows).T
    table = table[jax.random.permutation(jax.random.fold_in(own, 1), rows)]
    rotation = jax.random.randint(jax.random.fold_in(own, 2), (rows, 1), 0, top)
    return jnp.take_along_axis(table, (jnp.arange(top)[None, :] + rotation) % top, axis=1)


def load_shares(count, total, bound, lean, full):
    portions = [(1 << 20) // math.isqrt(rank ** lean) + 1 for rank in range(1, count + 1)]
    largest = bound if full else min(bound, max(-(-total // count), total * portions[0] // sum(portions)))
    least = 1 if total - largest >= count - 1 else 0
    holding, surplus = [largest] + [least] * (count - 1), total - largest - least * (count - 1)
    while surplus > 0:
        movable = [i for i in range(1, count) if holding[i] < largest] or [i for i in range(1, count) if holding[i] < bound]
        mass, left = sum([portions[i] for i in movable]), surplus
        for i in movable:
            extra = min(bound - holding[i], max(1, left * portions[i] // mass), surplus)
            holding[i] = holding[i] + extra
            surplus = surplus - extra
    return np.array(holding)


def centred(rng, shape, width, bound, cuts=(), held_as=jnp.bfloat16):
    array = jax.random.normal(rng, shape, jnp.float32) * width
    if len(cuts) > 0:
        array = block_levels(rng, shape, cuts, -0.22, 0.18) * array
    return jnp.clip(array, min=-bound, max=bound).astype(held_as)


def setup_inputs(seed: int = 0) -> dict:
    streams_of = jax.random.split(jax.random.key(seed), 9)
    displacement = centred(streams_of[0], (3, NZ, NX, NY), 1.0, 6.0, ((2, 8), (3, 4)), jnp.float32)
    previous = centred(streams_of[1], (3, NZ, NX, NY), 1.0, 6.0, ((2, 8), (3, 4)), jnp.float32)
    shear_coef = jnp.clip(jnp.exp(math.log(0.16) - 1.3862944 * jax.random.uniform(streams_of[2], (NZ, NX, NY), jnp.float32) ** block_levels(streams_of[2], (NZ, NX, NY), ((1, 8), (2, 4)), -0.2, 0.2)), 0.04, 0.16)
    bulk_coef = jnp.clip(jnp.exp(math.log(0.16) - 2.0794415 * jax.random.uniform(streams_of[3], (NZ, NX, NY), jnp.float32) ** block_levels(streams_of[3], (NZ, NX, NY), ((1, 8), (2, 4)), -0.2, 0.2)), 0.02, 0.16)
    cell_index = draw_cell_index(jax.random.fold_in(streams_of[8], 71), 0)
    archetype_id_keys = jax.random.split(jax.random.fold_in(streams_of[5], 1), BUILDINGS // BLD_DEV)
    archetype_id_turns = jax.random.permutation(jax.random.fold_in(streams_of[5], 3), BUILDINGS // BLD_DEV)
    archetype_id = jax.vmap(lambda own, number: deal_out(jax.random.fold_in(streams_of[5], 2), own, number, BLD_DEV, ARCHETYPES, 1, CAP, 2))(archetype_id_keys, archetype_id_turns).reshape((BUILDINGS, 1))
    transition = draw_transition(jax.random.fold_in(streams_of[8], 71), 0)
    forcing = centred(streams_of[7], (ARCHETYPES, 3, STATES), 0.5, 3.0, ((0, 32),), jnp.float32)
    return dict(displacement=displacement, previous=previous, shear_coef=shear_coef, bulk_coef=bulk_coef, cell_index=cell_index, archetype_id=archetype_id, transition=transition, forcing=forcing)


FIRST = ((-2, 1.0 / 12.0), (-1, -8.0 / 12.0), (1, 8.0 / 12.0), (2, -1.0 / 12.0))
SECOND = ((-2, -1.0 / 12.0), (-1, 16.0 / 12.0), (0, -30.0 / 12.0), (1, 16.0 / 12.0), (2, -1.0 / 12.0))
COMPONENT_AXIS = (1, 2, 0)


def pad_depth(padded):
    extent = padded.shape
    below = jnp.zeros((extent[0], 2, extent[2], extent[3]), padded.dtype)
    return jnp.concatenate([padded[:, 2:0:-1], padded, below], axis=1)


def shifted(volume, offsets):
    starts = [2 + offsets[0], 2 + offsets[1], 2 + offsets[2]]
    return volume[starts[0]:starts[0] + volume.shape[0] - 4,
                  starts[1]:starts[1] + volume.shape[1] - 4,
                  starts[2]:starts[2] + volume.shape[2] - 4]


def second_along(volume, main_axis):
    summed = None
    for amount, weight in SECOND:
        offsets = [0, 0, 0]
        offsets[main_axis] = amount
        term = weight * shifted(volume, offsets)
        summed = term if summed is None else summed + term
    return summed


def mixed_along(volume, main_axis, other_axis):
    summed = None
    for amount_a, weight_a in FIRST:
        for amount_b, weight_b in FIRST:
            offsets = [0, 0, 0]
            offsets[main_axis] = amount_a
            offsets[other_axis] = amount_b
            term = (weight_a * weight_b) * shifted(volume, offsets)
            summed = term if summed is None else summed + term
    return summed


def accelerate(padded, shear_coef, bulk_coef):
    results = []
    for component in range(3):
        volume = padded[component]
        main_axis = COMPONENT_AXIS[component]
        seconds = [second_along(volume, axis_a) for axis_a in range(3)]
        laplacian = seconds[0] + seconds[1] + seconds[2]
        divergence = seconds[main_axis]
        for partner in range(3):
            if partner != component:
                divergence = divergence + mixed_along(padded[partner], main_axis, COMPONENT_AXIS[partner])
        results.append(shear_coef * laplacian + bulk_coef * divergence)
    return jnp.stack(results)


def advance_grid(field, former, shear_coef, bulk_coef):
    padded = pad_depth(jnp.pad(field, ((0, 0), (0, 0), (2, 2), (2, 2))))
    return 2.0 * field - former + accelerate(padded, shear_coef, bulk_coef)


def ranks_of(members):
    order = jnp.arange(members.shape[0], dtype=jnp.int32)
    earlier = (members[:, None] == members[None, :]) & (order[None, :] < order[:, None])
    return jnp.sum(earlier.astype(jnp.int32), axis=1).astype(jnp.int32)


def reference(displacement, previous, shear_coef, bulk_coef, cell_index, archetype_id, transition, forcing):
    kinds = archetype_id[:, 0].astype(jnp.int32)
    position = lax.map(ranks_of, kinds.reshape(DEVICES, BLD_DEV)).reshape(-1).astype(jnp.int32)
    home_dev = (jnp.arange(BUILDINGS, dtype=jnp.int32) // BLD_DEV).astype(jnp.int32)
    states = jnp.zeros((BUILDINGS, STATES), jnp.float32)
    matrices = transition.astype(jnp.float32)
    field, former = displacement, previous
    for moment in range(COUPLINGS):
        for inner in range(EVERY):
            field, former = advance_grid(field, former, shear_coef, bulk_coef), field
        surface = field[:, 0].reshape(3, NX * NY)
        ground = jnp.take(surface, cell_index, axis=1)
        slots = jnp.zeros((ARCHETYPES, DEVICES, CAP, STATES), jnp.float32).at[kinds, home_dev, position].set(states)
        motion = jnp.zeros((ARCHETYPES, 3, DEVICES, CAP), jnp.float32).at[kinds, :, home_dev, position].set(ground.T)
        drive = motion[:, 0, :, :, None] * forcing[:, 0, None, None, :]
        drive = drive + motion[:, 1, :, :, None] * forcing[:, 1, None, None, :]
        drive = drive + motion[:, 2, :, :, None] * forcing[:, 2, None, None, :]
        for inner in range(SUB):
            rounded = lax.optimization_barrier(slots.astype(jnp.bfloat16)).astype(jnp.float32)
            slots = jnp.einsum("adck,ajk->adcj", rounded, matrices) + drive
        states = slots[kinds, home_dev, position]
    return field, states
```

```python
import functools

import jax
import jax.numpy as jnp
from jax import lax
from jax.experimental import pallas as pl
from jax.experimental.pallas import tpu as pltpu
from jax.sharding import PartitionSpec as P

COUPLINGS = 4
EVERY = 5
SUB = 6
UNIT = 8
EARLY = 5
CHUNK = 4
PLANES = 1
SCALE = 2.0 ** 60

A0, A1, A2 = -30.0 / 12.0, 16.0 / 12.0, -1.0 / 12.0
B1, B2 = 8.0 / 12.0, -1.0 / 12.0
DIRECTIONS = ((-1, 0), (1, 0), (0, -1), (0, 1), (-1, -1), (1, -1), (-1, 1), (1, 1))
MESH = pl.DeviceIdType.MESH


def first(plus1, minus1, plus2, minus2):
    return B1 * (plus1 - minus1) + B2 * (plus2 - minus2)


def city_kernel(
    d_hbm, p_hbm, sh_hbm, bk_hbm, cell_ref, kind_ref, t_hbm, f_hbm,
    f_ref, o_ref,
    raw, t_ref, force, sbuf, buf, sh_ref, bk_ref, ps, pr, gx, ht, th, hx, e_ref, s_ref, q_ref,
    vs, g_all, surf, hot, hotx, lhs, mot, fold,
    load_sem, give_send, give_recv, x_send, x_recv, y_send, y_recv,
    near_send, near_recv, hop_send, hop_recv, surf_send, surf_recv, back_send, back_recv,
):
    f32, bf16 = jnp.float32, jnp.bfloat16
    steps = COUPLINGS * EVERY
    cx, cy = sh_hbm.shape[1], sh_hbm.shape[2]
    nz = sh_hbm.shape[0]
    nr = nz // 2
    half = cy // 2
    rows = 2 * cx
    lo, hi = cx, cx + rows
    arch, width = t_hbm.shape[0], t_hbm.shape[1]
    count = kind_ref.shape[0]
    slab, gy = lax.axis_index("slab"), lax.axis_index("gy")
    slabs, gys = lax.axis_size("slab"), lax.axis_size("gy")
    pairs, pieces = slabs // 2, 2 * gys
    k, a = lax.div(slab, 2), lax.rem(slab, 2)
    hsel = lax.rem(a + gy, 2)
    piece = 2 * gy + hsel
    yb, cb = lax.div(gy, 2), lax.rem(gy, 2)
    chunks = nr // CHUNK
    groups = arch // UNIT
    units = groups * COUPLINGS

    def exists(dx, dy):
        x, y = k + dx, piece + dy
        return (x >= 0) & (x < pairs) & (y >= 0) & (y < pieces)

    def target(dx, dy):
        if dy == 0:
            return (2 * (k + dx) + a, gy)
        inner = (hsel == 0) if dy > 0 else (hsel == 1)
        return (2 * (k + dx) + jnp.where(inner, 1 - a, a), jnp.where(inner, gy, gy + dy))

    mate = (2 * k + 1 - a, gy)

    def load(i, src, dst):
        return pltpu.make_async_copy(src, dst, load_sem.at[i])

    loads = [
        load(0, d_hbm, raw.at[0:3]),
        load(1, p_hbm, raw.at[3:6]),
        load(2, sh_hbm, raw.at[6]),
        load(3, bk_hbm, raw.at[7]),
        load(4, t_hbm, t_ref),
        load(5, f_hbm, force),
    ]
    for one in loads:
        one.start()

    zero_tile = jnp.zeros((2, 3, nr + 4, cx, cy), f32)
    buf[:, :, :, 0:lo, :] = zero_tile
    buf[:, :, :, hi : hi + cx, :] = zero_tile
    pr[...] = jnp.zeros_like(pr)
    vs[...] = jnp.zeros_like(vs)
    g_rows = 2 * 3
    mot[...] = jnp.zeros_like(mot)

    barrier = pltpu.get_barrier_semaphore()

    def greet(device):
        pl.semaphore_signal(barrier, inc=1, device_id=device, device_id_type=MESH)

    def row_mates():
        for da in range(2):
            for dg in range(gys):
                if da or dg:
                    yield da, dg, (2 * k + lax.rem(a + da, 2), lax.rem(gy + dg, gys))

    for _, _, device in row_mates():
        greet(device)
    for dk in range(1, pairs):
        greet((2 * lax.rem(k + dk, pairs) + a, gy))
    for dx, dy in DIRECTIONS[4:]:
        @pl.when(exists(dx, dy))
        def _():
            greet(target(dx, dy))
    beside = [
        jnp.where(at > 0, 1, 0) + jnp.where(at < size - 1, 1, 0)
        for at, size in ((k, pairs), (piece, pieces))
    ]

    lane = lax.broadcasted_iota(jnp.int32, (cx, cy), 1)
    row = lax.broadcasted_iota(jnp.int32, (cx, cy), 0)
    left = lane < half

    def folded(near, far, second_half):
        if second_half:
            return jnp.where(left, pltpu.roll(near, half, 1), far)
        return jnp.where(left, near, pltpu.roll(far, half, 1))

    own = pl.ds(pl.multiple_of(cx * a, cx), cx)
    own_buf = pl.ds(pl.multiple_of(lo + cx * a, cx), cx)

    def kept_ref(i, r):
        if i < 3:
            return buf.at[0, i, r + 2, own_buf, :]
        if i < 6:
            return buf.at[1, i - 3, r + 2, own_buf, :]
        return (sh_ref if i == 6 else bk_ref).at[r, own, :]

    def give(i):
        if i < 3:
            dst = buf.at[0, i, 2 : nr + 2, own_buf, :]
        elif i < 6:
            dst = buf.at[1, i - 3, 2 : nr + 2, own_buf, :]
        else:
            dst = (sh_ref if i == 6 else bk_ref).at[:, own, :]
        return pltpu.make_async_remote_copy(
            src_ref=sbuf.at[i], dst_ref=dst, send_sem=give_send.at[i], recv_sem=give_recv.at[i],
            device_id=mate, device_id_type=MESH,
        )

    for i in range(8):
        if i in (0, 3, 6, 7):
            loads[{0: 0, 3: 1, 6: 2, 7: 3}[i]].wait()
        for r in range(nr):
            near, far = raw[i, r], raw[i, nz - 1 - r]
            lower, upper = folded(near, far, False), folded(near, far, True)
            kept_ref(i, r)[...] = jnp.where(hsel == 0, lower, upper)
            sbuf[i, r] = jnp.where(hsel == 0, upper, lower)
        if i == 0:
            corners = beside[0] * beside[1]
            pl.semaphore_wait(barrier, pieces - 1 + pairs - 1 + corners)
        give(i).start()

    ny = gys * cy
    cell = cell_ref[...]
    start = slab * cx
    along_x = jnp.zeros_like(cell)
    for i in range(1, cx):
        along_x = along_x + jnp.where(cell >= (start + i) * ny, 1, 0)
    column = cell - (start + along_x) * ny
    hotx[...] = jnp.where(
        lax.broadcasted_iota(jnp.int32, (cx, count), 0) == along_x, 1.0, 0.0
    )
    for i in range(ny // 128):
        hot[128 * i : 128 * (i + 1), :] = jnp.where(
            lax.broadcasted_iota(jnp.int32, (128, count), 0) + 128 * i == column, 1.0, 0.0
        ).astype(bf16)

    loads[4].wait()
    loads[5].wait()

    def face(dx, par, piece_r):
        mine = lo if dx < 0 else hi - 2
        theirs = hi if dx < 0 else lo - 2
        j = 0 if dx < 0 else 1
        span = pl.ds(2 + CHUNK * piece_r, CHUNK)
        return pltpu.make_async_remote_copy(
            src_ref=buf.at[par, :, span, mine : mine + 2, :],
            dst_ref=buf.at[par, :, span, theirs : theirs + 2, :],
            send_sem=x_send.at[par, j, piece_r], recv_sem=x_recv.at[par, j, piece_r],
            device_id=target(dx, 0), device_id_type=MESH,
        )

    def edge(j, par):
        dx, dy = DIRECTIONS[j]
        side = 1 if dy < 0 else 0
        if dx == 0:
            src = ps.at[par]
            dst = pr.at[par, side, :, lo:hi, :]
        else:
            mine = 0 if dx < 0 else rows - 2
            theirs = hi if dx < 0 else lo - 2
            src = ps.at[par, :, mine : mine + 2, :]
            dst = pr.at[par, side, :, theirs : theirs + 2, :]
        return pltpu.make_async_remote_copy(
            src_ref=src, dst_ref=dst, send_sem=y_send.at[par, j], recv_sem=y_recv.at[par, j],
            device_id=target(dx, dy), device_id_type=MESH,
        )

    def send_face(par, piece_r):
        for dx in (-1, 1):
            @pl.when(exists(dx, 0))
            def _():
                face(dx, par, piece_r).start()

    lane2 = lax.broadcasted_iota(jnp.int32, (rows, cy), 1)
    lanem = lax.rem(lane2, half)

    def send_edges(par):
        for c in range(3):
            packed = jnp.zeros((rows, cy), f32)
            for r in range(nr):
                turned = pltpu.roll(buf[par, c, r + 2, lo:hi, :], 2 + 4 * r, 1)
                packed = jnp.where((lanem >= 4 * r) & (lanem < 4 * r + 4), turned, packed)
            ps[par, c] = packed
        for j in range(2, 8):
            @pl.when(exists(*DIRECTIONS[j]))
            def _():
                edge(j, par).start()

    def wait_halos(par):
        for j, dx in enumerate((-1, 1)):
            @pl.when(exists(dx, 0))
            def _():
                for piece_r in range(chunks):
                    face(dx, par, piece_r).wait_send()
            @pl.when(exists(-dx, 0))
            def _():
                for piece_r in range(chunks):
                    face(dx, par, piece_r).wait_recv()
        for j in range(2, 8):
            dx, dy = DIRECTIONS[j]
            @pl.when(exists(dx, dy))
            def _():
                edge(j, par).wait_send()
            @pl.when(exists(-dx, -dy))
            def _():
                edge(j, par).wait_recv()

    left2 = lane2 < half
    sign = jnp.where(left2, 1.0, -1.0)
    sign1 = jnp.where(left, 1.0, -1.0)
    lm3 = lanem[None]
    lm1 = lax.rem(lane, half)[None]

    def depth_first(plus1, minus1, plus2, minus2, sgn):
        return (B1 * sgn) * (plus1 - minus1) + (B2 * sgn) * (plus2 - minus2)

    def along_y(core, halo, lm):
        return (
            pltpu.roll(jnp.where(lm < 1, halo, core), cy - 1, 2),
            pltpu.roll(jnp.where(lm >= half - 1, halo, core), 1, 2),
            pltpu.roll(jnp.where(lm < 2, halo, core), cy - 2, 2),
            pltpu.roll(jnp.where(lm >= half - 2, halo, core), 2, 2),
        )

    def ghosts(ref, index, span):
        mask = lax.broadcasted_iota(jnp.int32, (span.stop - span.start, cy), 1) < half
        at = lambda r: index + (r + 2, span, slice(None))
        ref[at(-1)] = jnp.where(mask, ref[at(1)], 0.0)
        ref[at(-2)] = jnp.where(mask, ref[at(2)], 0.0)
        ref[at(nr)] = pltpu.roll(ref[at(nr - 1)], half, 1)
        ref[at(nr + 1)] = pltpu.roll(ref[at(nr - 2)], half, 1)

    def grid_step(n, par):
        new = 1 - par
        wait_halos(par)

        ghosts(buf, (par, 0), slice(lo, hi))
        ghosts(buf, (par, 1), slice(lo, hi))
        ghosts(buf, (par, 2), slice(0, hi + cx))

        from_left = lax.rem(lane2, 4) < 2

        def joined(c, at, size):
            take = from_left if size == rows else from_left[0:size]
            return jnp.where(take, pr[par, 0, c, at : at + size, :], pr[par, 1, c, at : at + size, :])

        g = [joined(c, lo, rows) for c in range(3)]
        gx[lo:hi, :] = g[0]
        gx[0:lo, :] = joined(0, 0, cx)
        gx[hi : hi + cx, :] = joined(0, hi, cx)
        g_y = jnp.where(row < 4, joined(1, hi, cx), joined(1, 0, cx))
        a_g = first(
            gx[lo + 1 : hi + 1, :], gx[lo - 1 : hi - 1, :],
            gx[lo + 2 : hi + 2, :], gx[lo - 2 : hi - 2, :],
        )
        spot = lax.div(lanem, 4)
        turn = lambda v, by: pltpu.roll(v, by % cy, 1)
        h0_here = (~left2 & from_left) | (left2 & ~from_left)
        g2 = g[2]
        plus1 = jnp.where(spot == nr - 1, turn(g2, half), turn(g2, -4))
        plus2 = jnp.where(
            spot < nr - 2, turn(g2, -8),
            jnp.where(spot == nr - 2, turn(g2, -(half + 4)), turn(g2, -(half - 4))),
        )
        above = jnp.where(h0_here, turn(g2, -4), 0.0)
        minus1 = jnp.where(spot == 0, above, turn(g2, 4))
        minus2 = jnp.where(
            spot == 0, jnp.where(h0_here, turn(g2, -8), 0.0),
            jnp.where(spot == 1, jnp.where(h0_here, g2, 0.0), turn(g2, 8)),
        )
        t_g = a_g + depth_first(plus1, minus1, plus2, minus2, jnp.where(h0_here, 1.0, -1.0))
        for r in range(nr):
            back = (half - 2 - 4 * r) % cy
            for c in range(3):
                ht[c, r] = turn(g[c], back)
            th[r] = turn(t_g, back)
            hx[r] = turn(g_y, back)

        def u(c, r, shift, at, size=rows):
            return buf[par, c, pl.ds(r + 2 + shift, PLANES), at : at + size, :]

        def prepare(b, carry):
            r = b * PLANES
            x = first(u(0, r, 0, lo + 1), u(0, r, 0, lo - 1), u(0, r, 0, lo + 2), u(0, r, 0, lo - 2))
            y = first(*along_y(u(1, r, 0, lo), ht[1, pl.ds(r, PLANES)], lm3))
            z = depth_first(u(2, r, 1, lo), u(2, r, -1, lo), u(2, r, 2, lo), u(2, r, -2, lo), sign)
            e_ref[pl.ds(r + 2, PLANES)] = x + y
            s_ref[pl.ds(r, PLANES), lo:hi, :] = y + z
            q_ref[pl.ds(r, PLANES)] = x + z

            def mixed(comp, shift):
                return jnp.where(row[None] < 4, u(comp, r, shift, hi, cx), u(comp, r, shift, 0, cx))

            s_halo = first(*along_y(mixed(1, 0), hx[pl.ds(r, PLANES)], lm1)) + depth_first(
                mixed(2, 1), mixed(2, -1), mixed(2, 2), mixed(2, -2), sign1
            )
            s_ref[pl.ds(r, PLANES), 0:lo, :] = s_halo
            s_ref[pl.ds(r, PLANES), hi : hi + cx, :] = s_halo
            return carry

        lax.fori_loop(0, nr // PLANES, prepare, 0)
        ghosts(e_ref, (), slice(0, rows))

        def advance(b, carry):
            r = b * PLANES
            sh = sh_ref[pl.ds(r, PLANES)]
            bk = bk_ref[pl.ds(r, PLANES)]

            def s(at):
                return s_ref[pl.ds(r, PLANES), at : at + rows, :]

            def e(shift):
                return e_ref[pl.ds(r + 2 + shift, PLANES)]

            for c in range(3):
                mid = u(c, r, 0, lo)
                y = along_y(mid, ht[c, pl.ds(r, PLANES)], lm3)
                near = [u(c, r, 0, lo + 1) + u(c, r, 0, lo - 1), y[0] + y[1], u(c, r, 1, lo) + u(c, r, -1, lo)]
                far = [u(c, r, 0, lo + 2) + u(c, r, 0, lo - 2), y[2] + y[3], u(c, r, 2, lo) + u(c, r, -2, lo)]
                lap = (3.0 * A0) * mid + A1 * (near[0] + near[1] + near[2]) + A2 * (far[0] + far[1] + far[2])
                own_second = A0 * mid + A1 * near[c] + A2 * far[c]
                if c == 0:
                    cross = first(s(lo + 1), s(lo - 1), s(lo + 2), s(lo - 2))
                elif c == 1:
                    cross = first(*along_y(q_ref[pl.ds(r, PLANES)], th[pl.ds(r, PLANES)], lm3))
                else:
                    cross = depth_first(e(1), e(-1), e(2), e(-2), sign)
                acc = sh * lap + bk * (own_second + cross)
                place = (new, c, pl.ds(r + 2, PLANES), slice(lo, hi), slice(None))
                buf[place] = 2.0 * mid - buf[place] + acc
            return carry

        for piece_r in range(chunks):
            lax.fori_loop(piece_r * CHUNK // PLANES, (piece_r + 1) * CHUNK // PLANES, advance, 0)

            @pl.when(n < steps - 1)
            def _():
                send_face(new, piece_r)

        @pl.when(n < steps - 1)
        def _():
            send_edges(new)

    def surface_copy(moment, par, da, dg):
        to_a, to_g = lax.rem(a + da, 2), lax.rem(gy + dg, gys)
        at = pl.ds(pl.multiple_of(lo + cx * to_a, cx), cx)
        return pltpu.make_async_remote_copy(
            src_ref=buf.at[par, :, 2, at, :], dst_ref=surf.at[moment, piece],
            send_sem=surf_send.at[moment, gys * da + dg], recv_sem=surf_recv.at[moment, gys * da + dg],
            device_id=(2 * k + to_a, to_g), device_id_type=MESH,
        )

    def send_surface(moment, par):
        for da, dg, _ in row_mates():
            surface_copy(moment, par, da, dg).start()
        surf[moment, piece] = buf[par, :, 2, own_buf, :]

    def gather_motion(moment, par):
        for da, dg, _ in row_mates():
            surface_copy(moment, par, da, dg).wait()
        for j in range(gys):
            for c in range(3):
                even, odd = surf[moment, 2 * j, c], surf[moment, 2 * j + 1, c]
                table = jnp.where(left, even, pltpu.roll(odd, half, 1))
                for part in range(3):
                    piece_of = table.astype(bf16)
                    at = 24 * part + 8 * c
                    lhs[at : at + 8, 128 * j : 128 * (j + 1)] = piece_of.astype(f32)
                    table = table - piece_of.astype(f32)
        found = jnp.dot(lhs[...].astype(bf16), hot[...], preferred_element_type=f32)
        for c in range(3):
            value = found[8 * c : 8 * c + 8] + found[24 + 8 * c : 32 + 8 * c]
            value = value + found[48 + 8 * c : 56 + 8 * c]
            value = jnp.sum(value * hotx[...], axis=0, keepdims=True) * SCALE
            mot[moment, 2 * c : 2 * c + 1, :] = value
            mot[moment, 2 * c + 1 : 2 * c + 2, :] = value

    def unit_span(unit):
        return pl.ds(pl.multiple_of(lax.div(unit, COUPLINGS) * UNIT, UNIT), UNIT), COUPLINGS - 1 - lax.rem(unit, COUPLINGS)

    def g_copy(ref, device, send_sem, recv_sem):
        return pltpu.make_async_remote_copy(
            src_ref=ref, dst_ref=ref, send_sem=send_sem, recv_sem=recv_sem,
            device_id=device, device_id_type=MESH,
        )

    def spread(unit, dk):
        span, moment = unit_span(unit)
        ref = g_all.at[k, a, yb, cb, span, moment, 0:g_rows, :]
        return g_copy(
            ref, (2 * lax.rem(k + dk, pairs) + a, gy), near_send.at[unit, dk - 1], near_recv.at[unit, dk - 1]
        )

    y_mate = (slab, 2 * (1 - yb) + cb)
    c_mate = (slab, 2 * yb + 1 - cb)

    def hop(unit, phase, even):
        span, moment = unit_span(unit)
        tail = (span, moment, slice(0, g_rows), slice(None))
        if phase == 0:
            ref, device = g_all.at[(slice(None), a, yb, cb) + tail], mate if even else y_mate
        elif phase == 1 and even:
            ref, device = g_all.at[(slice(None), slice(None), yb, cb) + tail], y_mate
        elif phase == 1:
            ref, device = g_all.at[(slice(None), a, slice(None), cb) + tail], mate
        else:
            ref, device = g_all.at[(slice(None), slice(None), slice(None), cb) + tail], c_mate
        return g_copy(ref, device, hop_send.at[unit, phase], hop_recv.at[unit, phase])

    def respond(unit):
        stage = lax.rem(unit, COUPLINGS)
        group = lax.div(unit, COUPLINGS)

        @pl.when(stage == 0)
        def _():
            for i in range(UNIT):
                vs[i, 0:3, :] = force[group * UNIT + i] * (1.0 / SCALE)

        v = [vs[i] for i in range(UNIT)]
        total = list(v)
        for it in range(SUB):
            for i in range(UNIT):
                high = v[i].astype(bf16)
                low = (v[i] - high.astype(f32)).astype(bf16)
                both = jnp.concatenate([high, low], axis=0)
                got = lax.dot_general(
                    both, t_ref[group * UNIT + i], (((1,), (1,)), ((), ())), preferred_element_type=f32
                )
                v[i] = got[0:8] + got[8:16]
                if it < SUB - 1:
                    total[i] = total[i] + v[i]
        for i in range(UNIT):
            result = jnp.where(stage == 0, total[i], v[i])
            vs[i] = result
            for c in range(3):
                for h in range(2):
                    g_all[k, a, yb, cb, group * UNIT + i, COUPLINGS - 1 - stage, 2 * c + h : 2 * c + h + 1, :] = (
                        result[c : c + 1, 128 * h : 128 * (h + 1)]
                    )

    def tick(i):
        @pl.when(i < units)
        def _():
            respond(i)
            for dk in range(1, pairs):
                spread(i, dk).start()

        for phase in range(4):
            unit = i - 1 - phase
            for even in (True, False):
                @pl.when((unit >= 0) & (unit < units) & (lax.rem(unit + units, 2) == (0 if even else 1)))
                def _():
                    if phase == 0:
                        for dk in range(1, pairs):
                            spread(unit, dk).wait_recv()
                    else:
                        hop(unit, phase - 1, even).wait_recv()
                    if phase < 3:
                        hop(unit, phase, even).start()

    def body(i, carry):
        n = i - EARLY
        par = lax.rem(n + 2 * EARLY, 2)

        @pl.when(n == 0)
        def _():
            for j in range(8):
                give(j).wait()
            for piece_r in range(chunks):
                send_face(0, piece_r)
            send_edges(0)

        @pl.when(n >= 0)
        def _():
            grid_step(n, par)

        @pl.when((n >= 0) & (lax.rem(n + EARLY * EVERY, EVERY) == EVERY - 1))
        def _():
            send_surface(lax.div(n, EVERY), 1 - par)

        tick(i)

        @pl.when((n > 0) & (lax.rem(n + EARLY * EVERY, EVERY) == EVERY - 1) & (n < steps - 1))
        def _():
            gather_motion(lax.div(n, EVERY), 1 - par)
        return carry

    lax.fori_loop(0, EARLY + steps, body, 0)

    last = steps % 2
    theirs = pl.ds(pl.multiple_of(lo + cx * (1 - a), cx), cx)
    back = pltpu.make_async_remote_copy(
        src_ref=buf.at[last, :, 2 : nr + 2, theirs, :], dst_ref=fold,
        send_sem=back_send.at[0], recv_sem=back_recv.at[0], device_id=mate, device_id_type=MESH,
    )
    back.start()
    gather_motion(COUPLINGS - 1, last)

    for unit in range(units):
        for dk in range(1, pairs):
            spread(unit, dk).wait_send()
        for phase in range(3):
            hop(unit, phase, unit % 2 == 0).wait_send()

    table = g_all.reshape(slabs * gys * arch, COUPLINGS, 8, 128)
    row8 = lax.broadcasted_iota(jnp.int32, (8, 128), 0)

    def tile(j, carry):
        lanes = pl.ds(pl.multiple_of(128 * j, 128), 128)
        motion = [mot[m, :, lanes] for m in range(COUPLINGS)]

        def eight(i, motion):
            base = pl.multiple_of(128 * j + 8 * i, 8)
            out = [jnp.zeros((8, 128), f32)] * 2
            for b in range(8):
                kind = kind_ref[base + b]
                got = None
                for m in range(COUPLINGS):
                    term = jnp.broadcast_to(motion[m][:, b : b + 1], (8, 128)) * table[kind, m]
                    got = term if got is None else got + term
                got = jnp.where(row8 < g_rows, got, 0.0)
                got = got + pltpu.roll(got, 4, 0)
                got = got + pltpu.roll(got, 2, 0)
                moved = pltpu.roll(got, 1, 0)
                here, there = (got, moved) if b % 2 == 0 else (moved, got)
                out = [jnp.where(row8 == b, one, so_far) for one, so_far in zip((here, there), out)]
            o_ref[pl.ds(base, 8), 0:128] = out[0]
            o_ref[pl.ds(base, 8), 128:256] = out[1]
            return tuple(pltpu.roll(one, 120, 1) for one in motion)

        lax.fori_loop(0, 16, eight, tuple(motion))
        return carry

    lax.fori_loop(0, count // 128, tile, 0)

    back.wait()
    for c in range(3):
        for r in range(nr):
            mine, other = buf[last, c, r + 2, own_buf, :], fold[c, r]
            lower = jnp.where(hsel == 0, mine, other)
            upper = jnp.where(hsel == 0, other, mine)
            f_ref[c, r] = jnp.where(left, lower, pltpu.roll(upper, half, 1))
            f_ref[c, nz - 1 - r] = jnp.where(left, pltpu.roll(lower, half, 1), upper)


def per_device(
    displacement, previous, shear_coef, bulk_coef, cell_index, archetype_id, transition, forcing
):
    _, nz, cx, cy = displacement.shape
    arch, width, _ = transition.shape
    count = cell_index.shape[0]
    slabs, gys = lax.axis_size("slab"), lax.axis_size("gy")
    pairs, nr, rows = slabs // 2, nz // 2, 2 * cx
    tall = rows + 2 * cx
    units = arch // UNIT * COUPLINGS
    chunks = nr // CHUNK
    f32 = jnp.float32
    vmem, dma = pltpu.VMEM, pltpu.SemaphoreType.DMA
    whole = pl.BlockSpec(memory_space=pltpu.VMEM)
    away = pl.BlockSpec(memory_space=pl.ANY)
    return pl.pallas_call(
        city_kernel,
        out_shape=(
            jax.ShapeDtypeStruct(displacement.shape, f32),
            jax.ShapeDtypeStruct((count, width), f32),
        ),
        in_specs=[away] * 4 + [whole, pl.BlockSpec(memory_space=pltpu.SMEM), away, away],
        out_specs=(whole, whole),
        scratch_shapes=[
            vmem((8, nz, cx, cy), f32),
            vmem((arch, width, width), jnp.bfloat16),
            vmem((arch, 3, width), f32),
            vmem((8, nr, cx, cy), f32),
            vmem((2, 3, nr + 4, tall, cy), f32),
            vmem((nr, rows, cy), f32),
            vmem((nr, rows, cy), f32),
            vmem((2, 3, rows, cy), f32),
            vmem((2, 2, 3, tall, cy), f32),
            vmem((tall, cy), f32),
            vmem((3, nr, rows, cy), f32),
            vmem((nr, rows, cy), f32),
            vmem((nr, cx, cy), f32),
            vmem((nr + 4, rows, cy), f32),
            vmem((nr, tall, cy), f32),
            vmem((nr, rows, cy), f32),
            vmem((UNIT, 8, width), f32),
            vmem((pairs, 2, 2, gys // 2, arch, COUPLINGS, 8, 128), f32),
            vmem((COUPLINGS, 2 * gys, 3, cx, cy), f32),
            vmem((gys * cy, count), jnp.bfloat16),
            vmem((cx, count), f32),
            vmem((72, gys * cy), f32),
            vmem((COUPLINGS, 8, count), f32),
            vmem((3, nr, cx, cy), f32),
            dma((6,)),
            dma((8,)),
            dma((8,)),
            dma((2, 2, chunks)),
            dma((2, 2, chunks)),
            dma((2, 8)),
            dma((2, 8)),
            dma((units, pairs - 1)),
            dma((units, pairs - 1)),
            dma((units, 3)),
            dma((units, 3)),
            dma((COUPLINGS, 2 * gys)),
            dma((COUPLINGS, 2 * gys)),
            dma((1,)),
            dma((1,)),
        ],
        compiler_params=pltpu.CompilerParams(
            collective_id=0, has_side_effects=True, vmem_limit_bytes=60 * 1024 * 1024
        ),
    )(
        displacement, previous, shear_coef, bulk_coef, cell_index.reshape(1, count),
        archetype_id[:, 0], transition, forcing,
    )


def solution(mesh):
    in_specs = (
        P(None, None, "slab", "gy"),
        P(None, None, "slab", "gy"),
        P(None, "slab", "gy"),
        P(None, "slab", "gy"),
        P(("slab", "gy")),
        P(("slab", "gy"), None),
        P(("slab", "gy"), None, None),
        P(("slab", "gy"), None, None),
    )
    out_specs = (P(None, None, "slab", "gy"), P(("slab", "gy"), None))
    return jax.shard_map(
        per_device, mesh=mesh, in_specs=in_specs, out_specs=out_specs, check_vma=False
    )
```

```python
import functools

import jax
import jax.numpy as jnp
from jax import lax
from jax.experimental import pallas as pl
from jax.experimental.pallas import tpu as pltpu
from jax.sharding import PartitionSpec as P

COUPLINGS = 4
EVERY = 5
SUB = 6
UNIT = 8
EARLY = 5
CHUNK = 4
PREPARE = 16
ADVANCE = 4
SCALE = 2.0 ** 60
LEGS = ((0, 1), (2, 3), (4,))

A0, A1, A2 = -30.0 / 12.0, 16.0 / 12.0, -1.0 / 12.0
B1, B2 = 8.0 / 12.0, -1.0 / 12.0
DIRECTIONS = ((-1, 0), (1, 0), (0, -1), (0, 1), (-1, -1), (1, -1), (-1, 1), (1, 1))
MESH = pl.DeviceIdType.MESH


def first(plus1, minus1, plus2, minus2):
    return B1 * (plus1 - minus1) + B2 * (plus2 - minus2)


def city_kernel(
    d_hbm, p_hbm, sh_hbm, bk_hbm, cell_ref, kind_ref, t_hbm, f_hbm,
    f_ref, o_ref,
    raw, t_ref, force, sbuf, buf, sh_ref, bk_ref, ps, pr, gx, ht, th, hx, e_ref, s_ref, q_ref,
    vs, g_all, surf, hot, hotx, lhs, mot, fold,
    load_sem, give_send, give_recv, x_send, x_recv, y_send, y_recv,
    near_send, near_recv, hop_send, hop_recv, surf_send, surf_recv, back_send, back_recv,
):
    f32, bf16 = jnp.float32, jnp.bfloat16
    steps = COUPLINGS * EVERY
    cx, cy = sh_hbm.shape[1], sh_hbm.shape[2]
    nz = sh_hbm.shape[0]
    nr = nz // 2
    half = cy // 2
    rows = 2 * cx
    lo, hi = cx, cx + rows
    arch, width = t_hbm.shape[0], t_hbm.shape[1]
    count = kind_ref.shape[0]
    slab, gy = lax.axis_index("slab"), lax.axis_index("gy")
    slabs, gys = lax.axis_size("slab"), lax.axis_size("gy")
    pairs, pieces = slabs // 2, 2 * gys
    k, a = lax.div(slab, 2), lax.rem(slab, 2)
    hsel = lax.rem(a + gy, 2)
    piece = 2 * gy + hsel
    yb, cb = lax.div(gy, 2), lax.rem(gy, 2)
    chunks = nr // CHUNK
    groups = arch // UNIT
    units = groups * COUPLINGS

    def exists(dx, dy):
        x, y = k + dx, piece + dy
        return (x >= 0) & (x < pairs) & (y >= 0) & (y < pieces)

    def target(dx, dy):
        if dy == 0:
            return (2 * (k + dx) + a, gy)
        inner = (hsel == 0) if dy > 0 else (hsel == 1)
        return (2 * (k + dx) + jnp.where(inner, 1 - a, a), jnp.where(inner, gy, gy + dy))

    mate = (2 * k + 1 - a, gy)

    def load(i, src, dst):
        return pltpu.make_async_copy(src, dst, load_sem.at[i])

    loads = [
        load(0, d_hbm, raw.at[0:3]),
        load(1, p_hbm, raw.at[3:6]),
        load(2, sh_hbm, raw.at[6]),
        load(3, bk_hbm, raw.at[7]),
        load(4, t_hbm, t_ref),
        load(5, f_hbm, force),
    ]
    for one in loads:
        one.start()

    zero_tile = jnp.zeros((2, 3, nr + 4, cx, cy), f32)
    buf[:, :, :, 0:lo, :] = zero_tile
    buf[:, :, :, hi : hi + cx, :] = zero_tile
    pr[...] = jnp.zeros_like(pr)
    vs[...] = jnp.zeros_like(vs)
    g_rows = 2 * 3
    mot[...] = jnp.zeros_like(mot)

    barrier = pltpu.get_barrier_semaphore()

    def greet(device):
        pl.semaphore_signal(barrier, inc=1, device_id=device, device_id_type=MESH)

    def row_mates():
        for da in range(2):
            for dg in range(gys):
                if da or dg:
                    yield da, dg, (2 * k + lax.rem(a + da, 2), lax.rem(gy + dg, gys))

    for _, _, device in row_mates():
        greet(device)
    for dk in range(1, pairs):
        greet((2 * lax.rem(k + dk, pairs) + a, gy))
    for dx, dy in DIRECTIONS[4:]:
        @pl.when(exists(dx, dy))
        def _():
            greet(target(dx, dy))
    beside = [
        jnp.where(at > 0, 1, 0) + jnp.where(at < size - 1, 1, 0)
        for at, size in ((k, pairs), (piece, pieces))
    ]

    lane = lax.broadcasted_iota(jnp.int32, (cx, cy), 1)
    row = lax.broadcasted_iota(jnp.int32, (cx, cy), 0)
    left = lane < half

    def folded(near, far, second_half):
        if second_half:
            return jnp.where(left, pltpu.roll(near, half, 1), far)
        return jnp.where(left, near, pltpu.roll(far, half, 1))

    own = pl.ds(pl.multiple_of(cx * a, cx), cx)
    own_buf = pl.ds(pl.multiple_of(lo + cx * a, cx), cx)

    def kept_ref(i, r):
        if i < 3:
            return buf.at[0, i, r + 2, own_buf, :]
        if i < 6:
            return buf.at[1, i - 3, r + 2, own_buf, :]
        return (sh_ref if i == 6 else bk_ref).at[r, own, :]

    def give(i):
        if i < 3:
            dst = buf.at[0, i, 2 : nr + 2, own_buf, :]
        elif i < 6:
            dst = buf.at[1, i - 3, 2 : nr + 2, own_buf, :]
        else:
            dst = (sh_ref if i == 6 else bk_ref).at[:, own, :]
        return pltpu.make_async_remote_copy(
            src_ref=sbuf.at[i], dst_ref=dst, send_sem=give_send.at[i], recv_sem=give_recv.at[i],
            device_id=mate, device_id_type=MESH,
        )

    for i in range(8):
        if i in (0, 3, 6, 7):
            loads[{0: 0, 3: 1, 6: 2, 7: 3}[i]].wait()
        for r in range(nr):
            near, far = raw[i, r], raw[i, nz - 1 - r]
            lower, upper = folded(near, far, False), folded(near, far, True)
            kept_ref(i, r)[...] = jnp.where(hsel == 0, lower, upper)
            sbuf[i, r] = jnp.where(hsel == 0, upper, lower)
        if i == 0:
            corners = beside[0] * beside[1]
            pl.semaphore_wait(barrier, pieces - 1 + pairs - 1 + corners)
        give(i).start()

    ny = gys * cy
    cell = cell_ref[...]
    start = slab * cx
    along_x = jnp.zeros_like(cell)
    for i in range(1, cx):
        along_x = along_x + jnp.where(cell >= (start + i) * ny, 1, 0)
    column = cell - (start + along_x) * ny
    hotx[...] = jnp.where(
        lax.broadcasted_iota(jnp.int32, (cx, count), 0) == along_x, 1.0, 0.0
    )
    for i in range(ny // 128):
        hot[128 * i : 128 * (i + 1), :] = jnp.where(
            lax.broadcasted_iota(jnp.int32, (128, count), 0) + 128 * i == column, 1.0, 0.0
        ).astype(bf16)

    loads[4].wait()
    loads[5].wait()

    def face(dx, par, piece_r):
        mine = lo if dx < 0 else hi - 2
        theirs = hi if dx < 0 else lo - 2
        j = 0 if dx < 0 else 1
        span = pl.ds(2 + CHUNK * piece_r, CHUNK)
        return pltpu.make_async_remote_copy(
            src_ref=buf.at[par, :, span, mine : mine + 2, :],
            dst_ref=buf.at[par, :, span, theirs : theirs + 2, :],
            send_sem=x_send.at[par, j, piece_r], recv_sem=x_recv.at[par, j, piece_r],
            device_id=target(dx, 0), device_id_type=MESH,
        )

    def edge(j, par):
        dx, dy = DIRECTIONS[j]
        side = 1 if dy < 0 else 0
        if dx == 0:
            src = ps.at[par]
            dst = pr.at[par, side, :, lo:hi, :]
        else:
            mine = 0 if dx < 0 else rows - 2
            theirs = hi if dx < 0 else lo - 2
            src = ps.at[par, :, mine : mine + 2, :]
            dst = pr.at[par, side, :, theirs : theirs + 2, :]
        return pltpu.make_async_remote_copy(
            src_ref=src, dst_ref=dst, send_sem=y_send.at[par, j], recv_sem=y_recv.at[par, j],
            device_id=target(dx, dy), device_id_type=MESH,
        )

    def send_face(par, piece_r):
        for dx in (-1, 1):
            @pl.when(exists(dx, 0))
            def _():
                face(dx, par, piece_r).start()

    lane2 = lax.broadcasted_iota(jnp.int32, (rows, cy), 1)
    lanem = lax.rem(lane2, half)

    def send_edges(par):
        for c in range(3):
            packed = jnp.zeros((rows, cy), f32)
            for r in range(nr):
                turned = pltpu.roll(buf[par, c, r + 2, lo:hi, :], 2 + 4 * r, 1)
                packed = jnp.where((lanem >= 4 * r) & (lanem < 4 * r + 4), turned, packed)
            ps[par, c] = packed
        for j in range(2, 8):
            @pl.when(exists(*DIRECTIONS[j]))
            def _():
                edge(j, par).start()

    def wait_halos(par):
        for j, dx in enumerate((-1, 1)):
            @pl.when(exists(dx, 0))
            def _():
                for piece_r in range(chunks):
                    face(dx, par, piece_r).wait_send()
            @pl.when(exists(-dx, 0))
            def _():
                for piece_r in range(chunks):
                    face(dx, par, piece_r).wait_recv()
        for j in range(2, 8):
            dx, dy = DIRECTIONS[j]
            @pl.when(exists(dx, dy))
            def _():
                edge(j, par).wait_send()
            @pl.when(exists(-dx, -dy))
            def _():
                edge(j, par).wait_recv()

    left2 = lane2 < half
    sign = jnp.where(left2, 1.0, -1.0)
    sign1 = jnp.where(left, 1.0, -1.0)
    lm3 = lanem[None]
    lm1 = lax.rem(lane, half)[None]

    def depth_first(plus1, minus1, plus2, minus2, sgn):
        return (B1 * sgn) * (plus1 - minus1) + (B2 * sgn) * (plus2 - minus2)

    def along_y(core, halo, lm):
        return (
            pltpu.roll(jnp.where(lm < 1, halo, core), cy - 1, 2),
            pltpu.roll(jnp.where(lm >= half - 1, halo, core), 1, 2),
            pltpu.roll(jnp.where(lm < 2, halo, core), cy - 2, 2),
            pltpu.roll(jnp.where(lm >= half - 2, halo, core), 2, 2),
        )

    def ghosts(ref, index, span):
        mask = lax.broadcasted_iota(jnp.int32, (span.stop - span.start, cy), 1) < half
        at = lambda r: index + (r + 2, span, slice(None))
        ref[at(-1)] = jnp.where(mask, ref[at(1)], 0.0)
        ref[at(-2)] = jnp.where(mask, ref[at(2)], 0.0)
        ref[at(nr)] = pltpu.roll(ref[at(nr - 1)], half, 1)
        ref[at(nr + 1)] = pltpu.roll(ref[at(nr - 2)], half, 1)

    def grid_step(n, par):
        new = 1 - par
        wait_halos(par)

        ghosts(buf, (par, 0), slice(lo, hi))
        ghosts(buf, (par, 1), slice(lo, hi))
        ghosts(buf, (par, 2), slice(0, hi + cx))

        from_left = lax.rem(lane2, 4) < 2

        def joined(c, at, size):
            take = from_left if size == rows else from_left[0:size]
            return jnp.where(take, pr[par, 0, c, at : at + size, :], pr[par, 1, c, at : at + size, :])

        g = [joined(c, lo, rows) for c in range(3)]
        gx[lo:hi, :] = g[0]
        gx[0:lo, :] = joined(0, 0, cx)
        gx[hi : hi + cx, :] = joined(0, hi, cx)
        g_y = jnp.where(row < 4, joined(1, hi, cx), joined(1, 0, cx))
        a_g = first(
            gx[lo + 1 : hi + 1, :], gx[lo - 1 : hi - 1, :],
            gx[lo + 2 : hi + 2, :], gx[lo - 2 : hi - 2, :],
        )
        spot = lax.div(lanem, 4)
        turn = lambda v, by: pltpu.roll(v, by % cy, 1)
        h0_here = (~left2 & from_left) | (left2 & ~from_left)
        g2 = g[2]
        plus1 = jnp.where(spot == nr - 1, turn(g2, half), turn(g2, -4))
        plus2 = jnp.where(
            spot < nr - 2, turn(g2, -8),
            jnp.where(spot == nr - 2, turn(g2, -(half + 4)), turn(g2, -(half - 4))),
        )
        above = jnp.where(h0_here, turn(g2, -4), 0.0)
        minus1 = jnp.where(spot == 0, above, turn(g2, 4))
        minus2 = jnp.where(
            spot == 0, jnp.where(h0_here, turn(g2, -8), 0.0),
            jnp.where(spot == 1, jnp.where(h0_here, g2, 0.0), turn(g2, 8)),
        )
        t_g = a_g + depth_first(plus1, minus1, plus2, minus2, jnp.where(h0_here, 1.0, -1.0))
        for r in range(nr):
            back = (half - 2 - 4 * r) % cy
            for c in range(3):
                ht[c, r] = turn(g[c], back)
            th[r] = turn(t_g, back)
            hx[r] = turn(g_y, back)

        def reader(planes):
            def u(c, r, shift, at, size=rows):
                return buf[par, c, pl.ds(r + 2 + shift, planes), at : at + size, :]
            return u

        def prepare(b, carry):
            u, planes = reader(PREPARE), PREPARE
            r = b * PREPARE
            x = first(u(0, r, 0, lo + 1), u(0, r, 0, lo - 1), u(0, r, 0, lo + 2), u(0, r, 0, lo - 2))
            y = first(*along_y(u(1, r, 0, lo), ht[1, pl.ds(r, planes)], lm3))
            z = depth_first(u(2, r, 1, lo), u(2, r, -1, lo), u(2, r, 2, lo), u(2, r, -2, lo), sign)
            e_ref[pl.ds(r + 2, planes)] = x + y
            s_ref[pl.ds(r, planes), lo:hi, :] = y + z
            q_ref[pl.ds(r, planes)] = x + z

            def mixed(comp, shift):
                return jnp.where(row[None] < 4, u(comp, r, shift, hi, cx), u(comp, r, shift, 0, cx))

            s_halo = first(*along_y(mixed(1, 0), hx[pl.ds(r, planes)], lm1)) + depth_first(
                mixed(2, 1), mixed(2, -1), mixed(2, 2), mixed(2, -2), sign1
            )
            s_ref[pl.ds(r, planes), 0:lo, :] = s_halo
            s_ref[pl.ds(r, planes), hi : hi + cx, :] = s_halo
            return carry

        lax.fori_loop(0, nr // PREPARE, prepare, 0)
        ghosts(e_ref, (), slice(0, rows))

        def advance(b, carry):
            u, planes = reader(ADVANCE), ADVANCE
            r = b * ADVANCE
            sh = sh_ref[pl.ds(r, planes)]
            bk = bk_ref[pl.ds(r, planes)]

            def s(at):
                return s_ref[pl.ds(r, planes), at : at + rows, :]

            def e(shift):
                return e_ref[pl.ds(r + 2 + shift, planes)]

            for c in range(3):
                mid = u(c, r, 0, lo)
                y = along_y(mid, ht[c, pl.ds(r, planes)], lm3)
                near = [u(c, r, 0, lo + 1) + u(c, r, 0, lo - 1), y[0] + y[1], u(c, r, 1, lo) + u(c, r, -1, lo)]
                far = [u(c, r, 0, lo + 2) + u(c, r, 0, lo - 2), y[2] + y[3], u(c, r, 2, lo) + u(c, r, -2, lo)]
                lap = (3.0 * A0) * mid + A1 * (near[0] + near[1] + near[2]) + A2 * (far[0] + far[1] + far[2])
                own_second = A0 * mid + A1 * near[c] + A2 * far[c]
                if c == 0:
                    cross = first(s(lo + 1), s(lo - 1), s(lo + 2), s(lo - 2))
                elif c == 1:
                    cross = first(*along_y(q_ref[pl.ds(r, planes)], th[pl.ds(r, planes)], lm3))
                else:
                    cross = depth_first(e(1), e(-1), e(2), e(-2), sign)
                acc = sh * lap + bk * (own_second + cross)
                place = (new, c, pl.ds(r + 2, planes), slice(lo, hi), slice(None))
                buf[place] = 2.0 * mid - buf[place] + acc
            return carry

        for piece_r in range(chunks):
            lax.fori_loop(piece_r * CHUNK // ADVANCE, (piece_r + 1) * CHUNK // ADVANCE, advance, 0)

            @pl.when(n < steps - 1)
            def _():
                send_face(new, piece_r)

        @pl.when(n < steps - 1)
        def _():
            send_edges(new)

    def surface_copy(moment, par, da, dg):
        to_a, to_g = lax.rem(a + da, 2), lax.rem(gy + dg, gys)
        at = pl.ds(pl.multiple_of(lo + cx * to_a, cx), cx)
        return pltpu.make_async_remote_copy(
            src_ref=buf.at[par, :, 2, at, :], dst_ref=surf.at[moment, piece],
            send_sem=surf_send.at[moment, gys * da + dg], recv_sem=surf_recv.at[moment, gys * da + dg],
            device_id=(2 * k + to_a, to_g), device_id_type=MESH,
        )

    def send_surface(moment, par):
        for da, dg, _ in row_mates():
            surface_copy(moment, par, da, dg).start()
        surf[moment, piece] = buf[par, :, 2, own_buf, :]

    def gather_motion(moment, par):
        for da, dg, _ in row_mates():
            surface_copy(moment, par, da, dg).wait()
        for j in range(gys):
            for c in range(3):
                even, odd = surf[moment, 2 * j, c], surf[moment, 2 * j + 1, c]
                table = jnp.where(left, even, pltpu.roll(odd, half, 1))
                for part in range(3):
                    piece_of = table.astype(bf16)
                    at = 24 * part + 8 * c
                    lhs[at : at + 8, 128 * j : 128 * (j + 1)] = piece_of.astype(f32)
                    table = table - piece_of.astype(f32)
        found = jnp.dot(lhs[...].astype(bf16), hot[...], preferred_element_type=f32)
        for c in range(3):
            value = found[8 * c : 8 * c + 8] + found[24 + 8 * c : 32 + 8 * c]
            value = value + found[48 + 8 * c : 56 + 8 * c]
            value = jnp.sum(value * hotx[...], axis=0, keepdims=True) * SCALE
            mot[moment, 2 * c : 2 * c + 1, :] = value
            mot[moment, 2 * c + 1 : 2 * c + 2, :] = value

    def unit_span(unit):
        return pl.ds(pl.multiple_of(lax.div(unit, COUPLINGS) * UNIT, UNIT), UNIT), COUPLINGS - 1 - lax.rem(unit, COUPLINGS)

    def g_copy(ref, device, send_sem, recv_sem):
        return pltpu.make_async_remote_copy(
            src_ref=ref, dst_ref=ref, send_sem=send_sem, recv_sem=recv_sem,
            device_id=device, device_id_type=MESH,
        )

    def spread(unit, dk):
        span, moment = unit_span(unit)
        ref = g_all.at[k, a, yb, cb, span, moment, 0:g_rows, :]
        return g_copy(
            ref, (2 * lax.rem(k + dk, pairs) + a, gy), near_send.at[unit, dk - 1], near_recv.at[unit, dk - 1]
        )

    y_mate = (slab, 2 * (1 - yb) + cb)
    c_mate = (slab, 2 * yb + 1 - cb)

    def hop(unit, leg):
        span, moment = unit_span(unit)
        phase, even = divmod(leg, 2)
        if phase < 2:
            span = pl.ds(span.start + (0 if even == 0 else UNIT // 2), UNIT // 2)
        tail = (span, moment, slice(0, g_rows), slice(None))
        every = slice(None)
        if phase == 0:
            ref, device = g_all.at[(every, a, yb, cb) + tail], (mate, y_mate)[even]
        elif phase == 1:
            ref = g_all.at[((every, every, yb, cb) if even == 0 else (every, a, every, cb)) + tail]
            device = (y_mate, mate)[even]
        else:
            ref, device = g_all.at[(every, every, every, cb) + tail], c_mate
        return g_copy(ref, device, hop_send.at[unit, leg], hop_recv.at[unit, leg])

    def respond(unit):
        stage = lax.rem(unit, COUPLINGS)
        group = lax.div(unit, COUPLINGS)

        @pl.when(stage == 0)
        def _():
            for i in range(UNIT):
                vs[i, 0:3, :] = force[group * UNIT + i] * (1.0 / SCALE)

        v = [vs[i] for i in range(UNIT)]
        total = list(v)
        for it in range(SUB):
            for i in range(UNIT):
                high = v[i].astype(bf16)
                low = (v[i] - high.astype(f32)).astype(bf16)
                both = jnp.concatenate([high, low], axis=0)
                got = lax.dot_general(
                    both, t_ref[group * UNIT + i], (((1,), (1,)), ((), ())), preferred_element_type=f32
                )
                v[i] = got[0:8] + got[8:16]
                if it < SUB - 1:
                    total[i] = total[i] + v[i]
        for i in range(UNIT):
            result = jnp.where(stage == 0, total[i], v[i])
            vs[i] = result
            for c in range(3):
                for h in range(2):
                    g_all[k, a, yb, cb, group * UNIT + i, COUPLINGS - 1 - stage, 2 * c + h : 2 * c + h + 1, :] = (
                        result[c : c + 1, 128 * h : 128 * (h + 1)]
                    )

    def tick(i):
        @pl.when(i < units)
        def _():
            respond(i)
            for dk in range(1, pairs):
                spread(i, dk).start()

        for phase in range(4):
            unit = i - 1 - phase

            @pl.when((unit >= 0) & (unit < units))
            def _():
                if phase == 0:
                    for dk in range(1, pairs):
                        spread(unit, dk).wait_recv()
                else:
                    for leg in LEGS[phase - 1]:
                        hop(unit, leg).wait_recv()
                if phase < 3:
                    for leg in LEGS[phase]:
                        hop(unit, leg).start()

    def body(i, carry):
        n = i - EARLY
        par = lax.rem(n + 2 * EARLY, 2)

        @pl.when(n == 0)
        def _():
            for j in range(8):
                give(j).wait()
            for piece_r in range(chunks):
                send_face(0, piece_r)
            send_edges(0)

        @pl.when(n >= 0)
        def _():
            grid_step(n, par)

        @pl.when((n >= 0) & (lax.rem(n + EARLY * EVERY, EVERY) == EVERY - 1))
        def _():
            send_surface(lax.div(n, EVERY), 1 - par)

        tick(i)

        @pl.when((n > 0) & (lax.rem(n + EARLY * EVERY, EVERY) == EVERY - 1) & (n < steps - 1))
        def _():
            gather_motion(lax.div(n, EVERY), 1 - par)
        return carry

    lax.fori_loop(0, EARLY + steps, body, 0)

    last = steps % 2
    theirs = pl.ds(pl.multiple_of(lo + cx * (1 - a), cx), cx)
    back = pltpu.make_async_remote_copy(
        src_ref=buf.at[last, :, 2 : nr + 2, theirs, :], dst_ref=fold,
        send_sem=back_send.at[0], recv_sem=back_recv.at[0], device_id=mate, device_id_type=MESH,
    )
    back.start()
    gather_motion(COUPLINGS - 1, last)

    for unit in range(units):
        for dk in range(1, pairs):
            spread(unit, dk).wait_send()
        for leg in range(5):
            hop(unit, leg).wait_send()

    table = g_all.reshape(slabs * gys * arch, COUPLINGS, 8, 128)
    row8 = lax.broadcasted_iota(jnp.int32, (8, 128), 0)

    def tile(j, carry):
        lanes = pl.ds(pl.multiple_of(128 * j, 128), 128)
        motion = [mot[m, :, lanes] for m in range(COUPLINGS)]

        for i in range(16):
            base = pl.multiple_of(128 * j + 8 * i, 8)
            out = [jnp.zeros((8, 128), f32)] * 2
            for b in range(8):
                kind = kind_ref[128 * j + 8 * i + b]
                got = None
                for m in range(COUPLINGS):
                    at = 8 * i + b
                    term = jnp.broadcast_to(motion[m][:, at : at + 1], (8, 128)) * table[kind, m]
                    got = term if got is None else got + term
                got = jnp.where(row8 < g_rows, got, 0.0)
                got = got + pltpu.roll(got, 4, 0)
                got = got + pltpu.roll(got, 2, 0)
                moved = pltpu.roll(got, 1, 0)
                here, there = (got, moved) if b % 2 == 0 else (moved, got)
                out = [jnp.where(row8 == b, one, so_far) for one, so_far in zip((here, there), out)]
            o_ref[pl.ds(base, 8), 0:128] = out[0]
            o_ref[pl.ds(base, 8), 128:256] = out[1]
        return carry

    lax.fori_loop(0, count // 128, tile, 0)

    back.wait()
    for c in range(3):
        for r in range(nr):
            mine, other = buf[last, c, r + 2, own_buf, :], fold[c, r]
            lower = jnp.where(hsel == 0, mine, other)
            upper = jnp.where(hsel == 0, other, mine)
            f_ref[c, r] = jnp.where(left, lower, pltpu.roll(upper, half, 1))
            f_ref[c, nz - 1 - r] = jnp.where(left, pltpu.roll(lower, half, 1), upper)


def per_device(
    displacement, previous, shear_coef, bulk_coef, cell_index, archetype_id, transition, forcing
):
    _, nz, cx, cy = displacement.shape
    arch, width, _ = transition.shape
    count = cell_index.shape[0]
    slabs, gys = lax.axis_size("slab"), lax.axis_size("gy")
    pairs, nr, rows = slabs // 2, nz // 2, 2 * cx
    tall = rows + 2 * cx
    units = arch // UNIT * COUPLINGS
    chunks = nr // CHUNK
    f32 = jnp.float32
    vmem, dma = pltpu.VMEM, pltpu.SemaphoreType.DMA
    whole = pl.BlockSpec(memory_space=pltpu.VMEM)
    away = pl.BlockSpec(memory_space=pl.ANY)
    return pl.pallas_call(
        city_kernel,
        out_shape=(
            jax.ShapeDtypeStruct(displacement.shape, f32),
            jax.ShapeDtypeStruct((count, width), f32),
        ),
        in_specs=[away] * 4 + [whole, pl.BlockSpec(memory_space=pltpu.SMEM), away, away],
        out_specs=(whole, whole),
        scratch_shapes=[
            vmem((8, nz, cx, cy), f32),
            vmem((arch, width, width), jnp.bfloat16),
            vmem((arch, 3, width), f32),
            vmem((8, nr, cx, cy), f32),
            vmem((2, 3, nr + 4, tall, cy), f32),
            vmem((nr, rows, cy), f32),
            vmem((nr, rows, cy), f32),
            vmem((2, 3, rows, cy), f32),
            vmem((2, 2, 3, tall, cy), f32),
            vmem((tall, cy), f32),
            vmem((3, nr, rows, cy), f32),
            vmem((nr, rows, cy), f32),
            vmem((nr, cx, cy), f32),
            vmem((nr + 4, rows, cy), f32),
            vmem((nr, tall, cy), f32),
            vmem((nr, rows, cy), f32),
            vmem((UNIT, 8, width), f32),
            vmem((pairs, 2, 2, gys // 2, arch, COUPLINGS, 8, 128), f32),
            vmem((COUPLINGS, 2 * gys, 3, cx, cy), f32),
            vmem((gys * cy, count), jnp.bfloat16),
            vmem((cx, count), f32),
            vmem((72, gys * cy), f32),
            vmem((COUPLINGS, 8, count), f32),
            vmem((3, nr, cx, cy), f32),
            dma((6,)),
            dma((8,)),
            dma((8,)),
            dma((2, 2, chunks)),
            dma((2, 2, chunks)),
            dma((2, 8)),
            dma((2, 8)),
            dma((units, pairs - 1)),
            dma((units, pairs - 1)),
            dma((units, 5)),
            dma((units, 5)),
            dma((COUPLINGS, 2 * gys)),
            dma((COUPLINGS, 2 * gys)),
            dma((1,)),
            dma((1,)),
        ],
        compiler_params=pltpu.CompilerParams(
            collective_id=0, has_side_effects=True, vmem_limit_bytes=60 * 1024 * 1024
        ),
    )(
        displacement, previous, shear_coef, bulk_coef, cell_index.reshape(1, count),
        archetype_id[:, 0], transition, forcing,
    )


def solution(mesh):
    in_specs = (
        P(None, None, "slab", "gy"),
        P(None, None, "slab", "gy"),
        P(None, "slab", "gy"),
        P(None, "slab", "gy"),
        P(("slab", "gy")),
        P(("slab", "gy"), None),
        P(("slab", "gy"), None, None),
        P(("slab", "gy"), None, None),
    )
    out_specs = (P(None, None, "slab", "gy"), P(("slab", "gy"), None))
    return jax.shard_map(
        per_device, mesh=mesh, in_specs=in_specs, out_specs=out_specs, check_vma=False
    )
```

```python
import functools

import jax
import jax.numpy as jnp
from jax import lax
from jax.experimental import pallas as pl
from jax.experimental.pallas import tpu as pltpu
from jax.sharding import PartitionSpec as P

COUPLINGS = 4
EVERY = 5
SUB = 6
UNIT = 8
EARLY = 5
CHUNK = 8
FACE = 4
ADVANCE = 4
SCALE = 2.0 ** 60
LEGS = ((0, 1), (2, 3), (4,))

A0, A1, A2 = -30.0 / 12.0, 16.0 / 12.0, -1.0 / 12.0
B1, B2 = 8.0 / 12.0, -1.0 / 12.0
DIRECTIONS = ((-1, 0), (1, 0), (0, -1), (0, 1), (-1, -1), (1, -1), (-1, 1), (1, 1))
MESH = pl.DeviceIdType.MESH


def first(plus1, minus1, plus2, minus2):
    return B1 * (plus1 - minus1) + B2 * (plus2 - minus2)


def city_kernel(
    d_hbm, p_hbm, sh_hbm, bk_hbm, cell_ref, kind_ref, t_hbm, f_hbm,
    f_ref, o_ref,
    raw, t_ref, force, sbuf, buf, sh_ref, bk_ref, ps, pr, gx, ht, th, hx, e_ref, s_ref, q_ref,
    vs, g_all, surf, hot, hotx, lhs, mot, fold,
    load_sem, give_send, give_recv, x_send, x_recv, y_send, y_recv,
    near_send, near_recv, hop_send, hop_recv, surf_send, surf_recv, back_send, back_recv,
):
    f32, bf16 = jnp.float32, jnp.bfloat16
    steps = COUPLINGS * EVERY
    cx, cy = sh_hbm.shape[1], sh_hbm.shape[2]
    nz = sh_hbm.shape[0]
    nr = nz // 2
    half = cy // 2
    rows = 2 * cx
    lo, hi = cx, cx + rows
    arch, width = t_hbm.shape[0], t_hbm.shape[1]
    count = kind_ref.shape[0]
    slab, gy = lax.axis_index("slab"), lax.axis_index("gy")
    slabs, gys = lax.axis_size("slab"), lax.axis_size("gy")
    pairs, pieces = slabs // 2, 2 * gys
    k, a = lax.div(slab, 2), lax.rem(slab, 2)
    hsel = lax.rem(a + gy, 2)
    piece = 2 * gy + hsel
    yb, cb = lax.div(gy, 2), lax.rem(gy, 2)
    chunks = nr // CHUNK
    groups = arch // UNIT
    units = groups * COUPLINGS

    def exists(dx, dy):
        x, y = k + dx, piece + dy
        return (x >= 0) & (x < pairs) & (y >= 0) & (y < pieces)

    def target(dx, dy):
        if dy == 0:
            return (2 * (k + dx) + a, gy)
        inner = (hsel == 0) if dy > 0 else (hsel == 1)
        return (2 * (k + dx) + jnp.where(inner, 1 - a, a), jnp.where(inner, gy, gy + dy))

    mate = (2 * k + 1 - a, gy)

    def load(i, src, dst):
        return pltpu.make_async_copy(src, dst, load_sem.at[i])

    loads = [
        load(0, d_hbm, raw.at[0:3]),
        load(1, p_hbm, raw.at[3:6]),
        load(2, sh_hbm, raw.at[6]),
        load(3, bk_hbm, raw.at[7]),
        load(4, t_hbm, t_ref),
        load(5, f_hbm, force),
    ]
    for one in loads:
        one.start()

    zero_tile = jnp.zeros((2, 3, nr + 4, cx, cy), f32)
    buf[:, :, :, 0:lo, :] = zero_tile
    buf[:, :, :, hi : hi + cx, :] = zero_tile
    pr[...] = jnp.zeros_like(pr)
    vs[...] = jnp.zeros_like(vs)
    g_rows = 2 * 3
    mot[...] = jnp.zeros_like(mot)

    barrier = pltpu.get_barrier_semaphore()

    def greet(device):
        pl.semaphore_signal(barrier, inc=1, device_id=device, device_id_type=MESH)

    def row_mates():
        for da in range(2):
            for dg in range(gys):
                if da or dg:
                    yield da, dg, (2 * k + lax.rem(a + da, 2), lax.rem(gy + dg, gys))

    for _, _, device in row_mates():
        greet(device)
    for dk in range(1, pairs):
        greet((2 * lax.rem(k + dk, pairs) + a, gy))
    for dx, dy in DIRECTIONS[4:]:
        @pl.when(exists(dx, dy))
        def _():
            greet(target(dx, dy))
    beside = [
        jnp.where(at > 0, 1, 0) + jnp.where(at < size - 1, 1, 0)
        for at, size in ((k, pairs), (piece, pieces))
    ]

    lane = lax.broadcasted_iota(jnp.int32, (cx, cy), 1)
    row = lax.broadcasted_iota(jnp.int32, (cx, cy), 0)
    left = lane < half

    def folded(near, far, second_half):
        if second_half:
            return jnp.where(left, pltpu.roll(near, half, 1), far)
        return jnp.where(left, near, pltpu.roll(far, half, 1))

    own = pl.ds(pl.multiple_of(cx * a, cx), cx)
    own_buf = pl.ds(pl.multiple_of(lo + cx * a, cx), cx)

    def kept_ref(i, r):
        if i < 3:
            return buf.at[0, i, r + 2, own_buf, :]
        if i < 6:
            return buf.at[1, i - 3, r + 2, own_buf, :]
        return (sh_ref if i == 6 else bk_ref).at[r, own, :]

    def give(i):
        if i < 3:
            dst = buf.at[0, i, 2 : nr + 2, own_buf, :]
        elif i < 6:
            dst = buf.at[1, i - 3, 2 : nr + 2, own_buf, :]
        else:
            dst = (sh_ref if i == 6 else bk_ref).at[:, own, :]
        return pltpu.make_async_remote_copy(
            src_ref=sbuf.at[i], dst_ref=dst, send_sem=give_send.at[i], recv_sem=give_recv.at[i],
            device_id=mate, device_id_type=MESH,
        )

    for i in range(8):
        if i in (0, 3, 6, 7):
            loads[{0: 0, 3: 1, 6: 2, 7: 3}[i]].wait()
        for r in range(nr):
            near, far = raw[i, r], raw[i, nz - 1 - r]
            lower, upper = folded(near, far, False), folded(near, far, True)
            kept_ref(i, r)[...] = jnp.where(hsel == 0, lower, upper)
            sbuf[i, r] = jnp.where(hsel == 0, upper, lower)
        if i == 0:
            corners = beside[0] * beside[1]
            pl.semaphore_wait(barrier, pieces - 1 + pairs - 1 + corners)
        give(i).start()

    ny = gys * cy
    cell = cell_ref[...]
    start = slab * cx
    along_x = jnp.zeros_like(cell)
    for i in range(1, cx):
        along_x = along_x + jnp.where(cell >= (start + i) * ny, 1, 0)
    column = cell - (start + along_x) * ny
    hotx[...] = jnp.where(
        lax.broadcasted_iota(jnp.int32, (cx, count), 0) == along_x, 1.0, 0.0
    )
    for i in range(ny // 128):
        hot[128 * i : 128 * (i + 1), :] = jnp.where(
            lax.broadcasted_iota(jnp.int32, (128, count), 0) + 128 * i == column, 1.0, 0.0
        ).astype(bf16)

    loads[4].wait()
    loads[5].wait()

    def face(dx, par, piece_r):
        mine = lo if dx < 0 else hi - 2
        theirs = hi if dx < 0 else lo - 2
        j = 0 if dx < 0 else 1
        span = pl.ds(2 + FACE * piece_r, FACE)
        return pltpu.make_async_remote_copy(
            src_ref=buf.at[par, :, span, mine : mine + 2, :],
            dst_ref=buf.at[par, :, span, theirs : theirs + 2, :],
            send_sem=x_send.at[par, j, piece_r], recv_sem=x_recv.at[par, j, piece_r],
            device_id=target(dx, 0), device_id_type=MESH,
        )

    def edge(j, par, piece_r):
        dx, dy = DIRECTIONS[j]
        side = 1 if dy < 0 else 0
        if dx == 0:
            src = ps.at[par, piece_r]
            dst = pr.at[par, piece_r, side, :, lo:hi, :]
        else:
            mine = 0 if dx < 0 else rows - 2
            theirs = hi if dx < 0 else lo - 2
            src = ps.at[par, piece_r, :, mine : mine + 2, :]
            dst = pr.at[par, piece_r, side, :, theirs : theirs + 2, :]
        return pltpu.make_async_remote_copy(
            src_ref=src, dst_ref=dst, send_sem=y_send.at[par, piece_r, j], recv_sem=y_recv.at[par, piece_r, j],
            device_id=target(dx, dy), device_id_type=MESH,
        )

    def send_face(par, piece_r):
        for dx in (-1, 1):
            @pl.when(exists(dx, 0))
            def _():
                face(dx, par, piece_r).start()

    lane2 = lax.broadcasted_iota(jnp.int32, (rows, cy), 1)
    lanem = lax.rem(lane2, half)

    def send_edges(par, piece_r):
        for c in range(3):
            packed = jnp.zeros((rows, cy), f32)
            for r in range(CHUNK * piece_r, CHUNK * (piece_r + 1)):
                turned = pltpu.roll(buf[par, c, r + 2, lo:hi, :], 2 + 4 * r, 1)
                packed = jnp.where((lanem >= 4 * r) & (lanem < 4 * r + 4), turned, packed)
            ps[par, piece_r, c] = packed
        for j in range(2, 8):
            @pl.when(exists(*DIRECTIONS[j]))
            def _():
                edge(j, par, piece_r).start()

    def wait_halos(par, piece_r):
        for j, dx in enumerate((-1, 1)):
            parts = range(piece_r * CHUNK // FACE, (piece_r + 1) * CHUNK // FACE)
            @pl.when(exists(dx, 0))
            def _():
                for part in parts:
                    face(dx, par, part).wait_send()
            @pl.when(exists(-dx, 0))
            def _():
                for part in parts:
                    face(dx, par, part).wait_recv()
        for j in range(2, 8):
            dx, dy = DIRECTIONS[j]
            @pl.when(exists(dx, dy))
            def _():
                edge(j, par, piece_r).wait_send()
            @pl.when(exists(-dx, -dy))
            def _():
                edge(j, par, piece_r).wait_recv()

    left2 = lane2 < half
    sign = jnp.where(left2, 1.0, -1.0)
    sign1 = jnp.where(left, 1.0, -1.0)
    lm3 = lanem[None]
    lm1 = lax.rem(lane, half)[None]

    def depth_first(plus1, minus1, plus2, minus2, sgn):
        return (B1 * sgn) * (plus1 - minus1) + (B2 * sgn) * (plus2 - minus2)

    def along_y(core, halo, lm):
        return (
            pltpu.roll(jnp.where(lm < 1, halo, core), cy - 1, 2),
            pltpu.roll(jnp.where(lm >= half - 1, halo, core), 1, 2),
            pltpu.roll(jnp.where(lm < 2, halo, core), cy - 2, 2),
            pltpu.roll(jnp.where(lm >= half - 2, halo, core), 2, 2),
        )

    def ghosts(ref, index, span, top):
        at = lambda r: index + (r + 2, span, slice(None))
        if top:
            mask = lax.broadcasted_iota(jnp.int32, (span.stop - span.start, cy), 1) < half
            ref[at(-1)] = jnp.where(mask, ref[at(1)], 0.0)
            ref[at(-2)] = jnp.where(mask, ref[at(2)], 0.0)
        else:
            ref[at(nr)] = pltpu.roll(ref[at(nr - 1)], half, 1)
            ref[at(nr + 1)] = pltpu.roll(ref[at(nr - 2)], half, 1)

    from_left = lax.rem(lane2, 4) < 2
    spot = lax.div(lanem, 4)
    turn = lambda v, by: pltpu.roll(v, by % cy, 1)
    h0_here = (~left2 & from_left) | (left2 & ~from_left)

    def grid_step(n, par):
        new = 1 - par

        def received(c, at, size, piece_r):
            return jnp.where(
                from_left[0:size], pr[par, piece_r, 0, c, at : at + size, :],
                pr[par, piece_r, 1, c, at : at + size, :],
            )

        def joined(c, at, size, last_piece):
            got = received(c, at, size, 0)
            for piece_r in range(1, last_piece + 1):
                got = jnp.where(spot[0:size] < CHUNK * piece_r, got, received(c, at, size, piece_r))
            return got

        def unpack(piece_r, r0, r1, t0, t1):
            g = [joined(c, lo, rows, piece_r) for c in range(3)]
            gx[lo:hi, :] = g[0]
            gx[0:lo, :] = joined(0, 0, cx, piece_r)
            gx[hi : hi + cx, :] = joined(0, hi, cx, piece_r)
            g_y = jnp.where(row < 4, joined(1, hi, cx, piece_r), joined(1, 0, cx, piece_r))
            a_g = first(
                gx[lo + 1 : hi + 1, :], gx[lo - 1 : hi - 1, :],
                gx[lo + 2 : hi + 2, :], gx[lo - 2 : hi - 2, :],
            )
            g2 = g[2]
            plus1, plus2, minus1, minus2 = turn(g2, -4), turn(g2, -8), turn(g2, 4), turn(g2, 8)
            if t0 == 0:
                minus1 = jnp.where(spot == 0, jnp.where(h0_here, turn(g2, -4), 0.0), minus1)
                minus2 = jnp.where(
                    spot == 0, jnp.where(h0_here, turn(g2, -8), 0.0),
                    jnp.where(spot == 1, jnp.where(h0_here, g2, 0.0), minus2),
                )
            if t1 == nr:
                plus1 = jnp.where(spot == nr - 1, turn(g2, half), plus1)
                plus2 = jnp.where(
                    spot < nr - 2, plus2,
                    jnp.where(spot == nr - 2, turn(g2, -(half + 4)), turn(g2, -(half - 4))),
                )
            t_g = a_g + depth_first(plus1, minus1, plus2, minus2, jnp.where(h0_here, 1.0, -1.0))
            for r in range(r0, r1):
                back = (half - 2 - 4 * r) % cy
                for c in range(3):
                    ht[c, r] = turn(g[c], back)
                hx[r] = turn(g_y, back)
            for r in range(t0, t1):
                th[r] = turn(t_g, (half - 2 - 4 * r) % cy)

        def reader(planes):
            def u(c, r, shift, at, size=rows):
                return buf[par, c, pl.ds(r + 2 + shift, planes), at : at + size, :]
            return u

        def prepare(r, planes):
            u = reader(planes)
            x = first(u(0, r, 0, lo + 1), u(0, r, 0, lo - 1), u(0, r, 0, lo + 2), u(0, r, 0, lo - 2))
            y = first(*along_y(u(1, r, 0, lo), ht[1, pl.ds(r, planes)], lm3))
            z = depth_first(u(2, r, 1, lo), u(2, r, -1, lo), u(2, r, 2, lo), u(2, r, -2, lo), sign)
            e_ref[pl.ds(r + 2, planes)] = x + y
            s_ref[pl.ds(r, planes), lo:hi, :] = y + z
            q_ref[pl.ds(r, planes)] = x + z

            def mixed(comp, shift):
                return jnp.where(row[None] < 4, u(comp, r, shift, hi, cx), u(comp, r, shift, 0, cx))

            s_halo = first(*along_y(mixed(1, 0), hx[pl.ds(r, planes)], lm1)) + depth_first(
                mixed(2, 1), mixed(2, -1), mixed(2, 2), mixed(2, -2), sign1
            )
            s_ref[pl.ds(r, planes), 0:lo, :] = s_halo
            s_ref[pl.ds(r, planes), hi : hi + cx, :] = s_halo

        def advance(b, carry):
            u, planes = reader(ADVANCE), ADVANCE
            r = b * ADVANCE
            sh = sh_ref[pl.ds(r, planes)]
            bk = bk_ref[pl.ds(r, planes)]

            def s(at):
                return s_ref[pl.ds(r, planes), at : at + rows, :]

            def e(shift):
                return e_ref[pl.ds(r + 2 + shift, planes)]

            for c in range(3):
                mid = u(c, r, 0, lo)
                y = along_y(mid, ht[c, pl.ds(r, planes)], lm3)
                near = [u(c, r, 0, lo + 1) + u(c, r, 0, lo - 1), y[0] + y[1], u(c, r, 1, lo) + u(c, r, -1, lo)]
                far = [u(c, r, 0, lo + 2) + u(c, r, 0, lo - 2), y[2] + y[3], u(c, r, 2, lo) + u(c, r, -2, lo)]
                lap = (3.0 * A0) * mid + A1 * (near[0] + near[1] + near[2]) + A2 * (far[0] + far[1] + far[2])
                own_second = A0 * mid + A1 * near[c] + A2 * far[c]
                if c == 0:
                    cross = first(s(lo + 1), s(lo - 1), s(lo + 2), s(lo - 2))
                elif c == 1:
                    cross = first(*along_y(q_ref[pl.ds(r, planes)], th[pl.ds(r, planes)], lm3))
                else:
                    cross = depth_first(e(1), e(-1), e(2), e(-2), sign)
                acc = sh * lap + bk * (own_second + cross)
                place = (new, c, pl.ds(r + 2, planes), slice(lo, hi), slice(None))
                buf[place] = 2.0 * mid - buf[place] + acc
            return carry

        def share(stop):
            @pl.when(n < steps - 1)
            def _():
                send_face(new, stop // FACE - 1)
                if stop % CHUNK == 0:
                    send_edges(new, stop // CHUNK - 1)

        done, ready, known = 0, 0, 0
        for piece_r in range(chunks):
            wait_halos(par, piece_r)
            last_piece = piece_r == chunks - 1
            if piece_r == 0:
                for c, span in ((0, slice(lo, hi)), (1, slice(lo, hi)), (2, slice(0, hi + cx))):
                    ghosts(buf, (par, c), span, True)
            if last_piece:
                for c, span in ((0, slice(lo, hi)), (1, slice(lo, hi)), (2, slice(0, hi + cx))):
                    ghosts(buf, (par, c), span, False)
            upto = CHUNK * (piece_r + 1)
            safe = nr if last_piece else upto - 2
            unpack(piece_r, known, upto, ready, safe)
            prepare(ready, safe - ready)
            if piece_r == 0:
                ghosts(e_ref, (), slice(0, rows), True)
            if last_piece:
                ghosts(e_ref, (), slice(0, rows), False)
            known, ready = upto, safe
            limit = nr if last_piece else ADVANCE * ((safe - 2) // ADVANCE)
            while done < limit:
                stop = done + FACE
                lax.fori_loop(done // ADVANCE, stop // ADVANCE, advance, 0)
                share(stop)
                done = stop

    def surface_copy(moment, par, da, dg):
        to_a, to_g = lax.rem(a + da, 2), lax.rem(gy + dg, gys)
        at = pl.ds(pl.multiple_of(lo + cx * to_a, cx), cx)
        return pltpu.make_async_remote_copy(
            src_ref=buf.at[par, :, 2, at, :], dst_ref=surf.at[moment, piece],
            send_sem=surf_send.at[moment, gys * da + dg], recv_sem=surf_recv.at[moment, gys * da + dg],
            device_id=(2 * k + to_a, to_g), device_id_type=MESH,
        )

    def send_surface(moment, par):
        for da, dg, _ in row_mates():
            surface_copy(moment, par, da, dg).start()
        surf[moment, piece] = buf[par, :, 2, own_buf, :]

    def gather_motion(moment, par):
        for da, dg, _ in row_mates():
            surface_copy(moment, par, da, dg).wait()
        for j in range(gys):
            for c in range(3):
                even, odd = surf[moment, 2 * j, c], surf[moment, 2 * j + 1, c]
                table = jnp.where(left, even, pltpu.roll(odd, half, 1))
                for part in range(3):
                    piece_of = table.astype(bf16)
                    at = 24 * part + 8 * c
                    lhs[at : at + 8, 128 * j : 128 * (j + 1)] = piece_of.astype(f32)
                    table = table - piece_of.astype(f32)
        found = jnp.dot(lhs[...].astype(bf16), hot[...], preferred_element_type=f32)
        for c in range(3):
            value = found[8 * c : 8 * c + 8] + found[24 + 8 * c : 32 + 8 * c]
            value = value + found[48 + 8 * c : 56 + 8 * c]
            value = jnp.sum(value * hotx[...], axis=0, keepdims=True) * SCALE
            mot[moment, 2 * c : 2 * c + 1, :] = value
            mot[moment, 2 * c + 1 : 2 * c + 2, :] = value

    def unit_span(unit):
        return pl.ds(pl.multiple_of(lax.div(unit, COUPLINGS) * UNIT, UNIT), UNIT), COUPLINGS - 1 - lax.rem(unit, COUPLINGS)

    def g_copy(ref, device, send_sem, recv_sem):
        return pltpu.make_async_remote_copy(
            src_ref=ref, dst_ref=ref, send_sem=send_sem, recv_sem=recv_sem,
            device_id=device, device_id_type=MESH,
        )

    def spread(unit, dk):
        span, moment = unit_span(unit)
        ref = g_all.at[k, a, yb, cb, span, moment, 0:g_rows, :]
        return g_copy(
            ref, (2 * lax.rem(k + dk, pairs) + a, gy), near_send.at[unit, dk - 1], near_recv.at[unit, dk - 1]
        )

    y_mate = (slab, 2 * (1 - yb) + cb)
    c_mate = (slab, 2 * yb + 1 - cb)

    def hop(unit, leg):
        span, moment = unit_span(unit)
        phase, even = divmod(leg, 2)
        if phase < 2:
            span = pl.ds(span.start + (0 if even == 0 else UNIT // 2), UNIT // 2)
        tail = (span, moment, slice(0, g_rows), slice(None))
        every = slice(None)
        if phase == 0:
            ref, device = g_all.at[(every, a, yb, cb) + tail], (mate, y_mate)[even]
        elif phase == 1:
            ref = g_all.at[((every, every, yb, cb) if even == 0 else (every, a, every, cb)) + tail]
            device = (y_mate, mate)[even]
        else:
            ref, device = g_all.at[(every, every, every, cb) + tail], c_mate
        return g_copy(ref, device, hop_send.at[unit, leg], hop_recv.at[unit, leg])

    def respond(unit):
        stage = lax.rem(unit, COUPLINGS)
        group = lax.div(unit, COUPLINGS)

        @pl.when(stage == 0)
        def _():
            span = pl.ds(pl.multiple_of(group * UNIT, UNIT), UNIT)
            rows_of = [force[c, span, :] for c in range(3)]
            for i in range(UNIT):
                for c in range(3):
                    vs[i, c : c + 1, :] = rows_of[c][i : i + 1] * (1.0 / SCALE)

        v = [vs[i] for i in range(UNIT)]
        total = list(v)
        for it in range(SUB):
            for i in range(UNIT):
                high = v[i].astype(bf16)
                low = (v[i] - high.astype(f32)).astype(bf16)
                both = jnp.concatenate([high, low], axis=0)
                got = lax.dot_general(
                    both, t_ref[group * UNIT + i], (((1,), (1,)), ((), ())), preferred_element_type=f32
                )
                v[i] = got[0:8] + got[8:16]
                if it < SUB - 1:
                    total[i] = total[i] + v[i]
        for i in range(UNIT):
            result = jnp.where(stage == 0, total[i], v[i])
            vs[i] = result
            for c in range(3):
                for h in range(2):
                    g_all[k, a, yb, cb, group * UNIT + i, COUPLINGS - 1 - stage, 2 * c + h : 2 * c + h + 1, :] = (
                        result[c : c + 1, 128 * h : 128 * (h + 1)]
                    )

    def tick_links(i):
        for phase in range(5):
            unit = i - 1 - 2 * phase

            @pl.when((unit >= 0) & (unit < units))
            def _():
                if phase == 1:
                    for dk in range(1, pairs):
                        spread(unit, dk).wait_recv()
                elif phase > 1:
                    for leg in LEGS[phase - 2]:
                        hop(unit, leg).wait_recv()
                if phase == 0:
                    for dk in range(1, pairs):
                        spread(unit, dk).start()
                elif phase < 4:
                    for leg in LEGS[phase - 1]:
                        hop(unit, leg).start()

    def body(i, carry):
        n = i - EARLY
        par = lax.rem(n + 2 * EARLY, 2)

        @pl.when(n == 0)
        def _():
            for j in range(8):
                give(j).wait()
            for part in range(nr // FACE):
                send_face(0, part)
            for piece_r in range(chunks):
                send_edges(0, piece_r)

        @pl.when(n >= 0)
        def _():
            grid_step(n, par)

        @pl.when((n >= 0) & (lax.rem(n + EARLY * EVERY, EVERY) == EVERY - 1))
        def _():
            send_surface(lax.div(n, EVERY), 1 - par)

        tick_links(i)

        @pl.when(i < units)
        def _():
            respond(i)

        @pl.when((n > 0) & (lax.rem(n + EARLY * EVERY, EVERY) == EVERY - 1) & (n < steps - 1))
        def _():
            gather_motion(lax.div(n, EVERY), 1 - par)
        return carry

    lax.fori_loop(0, EARLY + steps, body, 0)

    last = steps % 2
    theirs = pl.ds(pl.multiple_of(lo + cx * (1 - a), cx), cx)
    back = pltpu.make_async_remote_copy(
        src_ref=buf.at[last, :, 2 : nr + 2, theirs, :], dst_ref=fold,
        send_sem=back_send.at[0], recv_sem=back_recv.at[0], device_id=mate, device_id_type=MESH,
    )
    back.start()
    gather_motion(COUPLINGS - 1, last)

    for unit in range(units):
        for dk in range(1, pairs):
            spread(unit, dk).wait_send()
        for leg in range(5):
            hop(unit, leg).wait_send()

    table = g_all.reshape(slabs * gys * arch, COUPLINGS, 8, 128)
    row8 = lax.broadcasted_iota(jnp.int32, (8, 128), 0)

    def tile(j, carry):
        lanes = pl.ds(pl.multiple_of(128 * j, 128), 128)
        motion = [mot[m, :, lanes] for m in range(COUPLINGS)]

        for i in range(16):
            base = pl.multiple_of(128 * j + 8 * i, 8)
            out = [jnp.zeros((8, 128), f32)] * 2
            for b in range(8):
                kind = kind_ref[128 * j + 8 * i + b]
                got = None
                for m in range(COUPLINGS):
                    at = 8 * i + b
                    term = jnp.broadcast_to(motion[m][:, at : at + 1], (8, 128)) * table[kind, m]
                    got = term if got is None else got + term
                got = jnp.where(row8 < g_rows, got, 0.0)
                got = got + pltpu.roll(got, 4, 0)
                got = got + pltpu.roll(got, 2, 0)
                moved = pltpu.roll(got, 1, 0)
                here, there = (got, moved) if b % 2 == 0 else (moved, got)
                out = [jnp.where(row8 == b, one, so_far) for one, so_far in zip((here, there), out)]
            o_ref[pl.ds(base, 8), 0:128] = out[0]
            o_ref[pl.ds(base, 8), 128:256] = out[1]
        return carry

    lax.fori_loop(0, count // 128, tile, 0)

    back.wait()
    for c in range(3):
        for r in range(nr):
            mine, other = buf[last, c, r + 2, own_buf, :], fold[c, r]
            lower = jnp.where(hsel == 0, mine, other)
            upper = jnp.where(hsel == 0, other, mine)
            f_ref[c, r] = jnp.where(left, lower, pltpu.roll(upper, half, 1))
            f_ref[c, nz - 1 - r] = jnp.where(left, pltpu.roll(lower, half, 1), upper)


def per_device(
    displacement, previous, shear_coef, bulk_coef, cell_index, archetype_id, transition, forcing
):
    _, nz, cx, cy = displacement.shape
    arch, width, _ = transition.shape
    count = cell_index.shape[0]
    slabs, gys = lax.axis_size("slab"), lax.axis_size("gy")
    pairs, nr, rows = slabs // 2, nz // 2, 2 * cx
    tall = rows + 2 * cx
    units = arch // UNIT * COUPLINGS
    chunks = nr // CHUNK
    f32 = jnp.float32
    vmem, dma = pltpu.VMEM, pltpu.SemaphoreType.DMA
    whole = pl.BlockSpec(memory_space=pltpu.VMEM)
    away = pl.BlockSpec(memory_space=pl.ANY)
    return pl.pallas_call(
        city_kernel,
        out_shape=(
            jax.ShapeDtypeStruct(displacement.shape, f32),
            jax.ShapeDtypeStruct((count, width), f32),
        ),
        in_specs=[away] * 4 + [whole, pl.BlockSpec(memory_space=pltpu.SMEM), away, away],
        out_specs=(whole, whole),
        scratch_shapes=[
            vmem((8, nz, cx, cy), f32),
            vmem((arch, width, width), jnp.bfloat16),
            vmem((3, arch, width), f32),
            vmem((8, nr, cx, cy), f32),
            vmem((2, 3, nr + 4, tall, cy), f32),
            vmem((nr, rows, cy), f32),
            vmem((nr, rows, cy), f32),
            vmem((2, chunks, 3, rows, cy), f32),
            vmem((2, chunks, 2, 3, tall, cy), f32),
            vmem((tall, cy), f32),
            vmem((3, nr, rows, cy), f32),
            vmem((nr, rows, cy), f32),
            vmem((nr, cx, cy), f32),
            vmem((nr + 4, rows, cy), f32),
            vmem((nr, tall, cy), f32),
            vmem((nr, rows, cy), f32),
            vmem((UNIT, 8, width), f32),
            vmem((pairs, 2, 2, gys // 2, arch, COUPLINGS, 8, 128), f32),
            vmem((COUPLINGS, 2 * gys, 3, cx, cy), f32),
            vmem((gys * cy, count), jnp.bfloat16),
            vmem((cx, count), f32),
            vmem((72, gys * cy), f32),
            vmem((COUPLINGS, 8, count), f32),
            vmem((3, nr, cx, cy), f32),
            dma((6,)),
            dma((8,)),
            dma((8,)),
            dma((2, 2, nr // FACE)),
            dma((2, 2, nr // FACE)),
            dma((2, chunks, 8)),
            dma((2, chunks, 8)),
            dma((units, pairs - 1)),
            dma((units, pairs - 1)),
            dma((units, 5)),
            dma((units, 5)),
            dma((COUPLINGS, 2 * gys)),
            dma((COUPLINGS, 2 * gys)),
            dma((1,)),
            dma((1,)),
        ],
        compiler_params=pltpu.CompilerParams(
            collective_id=0, has_side_effects=True, vmem_limit_bytes=60 * 1024 * 1024
        ),
    )(
        displacement, previous, shear_coef, bulk_coef, cell_index.reshape(1, count),
        archetype_id[:, 0], transition, forcing.transpose(1, 0, 2),
    )


def solution(mesh):
    in_specs = (
        P(None, None, "slab", "gy"),
        P(None, None, "slab", "gy"),
        P(None, "slab", "gy"),
        P(None, "slab", "gy"),
        P(("slab", "gy")),
        P(("slab", "gy"), None),
        P(("slab", "gy"), None, None),
        P(("slab", "gy"), None, None),
    )
    out_specs = (P(None, None, "slab", "gy"), P(("slab", "gy"), None))
    return jax.shard_map(
        per_device, mesh=mesh, in_specs=in_specs, out_specs=out_specs, check_vma=False
    )
```

```python
import functools

import jax
import jax.numpy as jnp
from jax import lax
from jax.experimental import pallas as pl
from jax.experimental.pallas import tpu as pltpu
from jax.sharding import PartitionSpec as P

COUPLINGS = 4
EVERY = 5
SUB = 6
UNIT = 8
EARLY = 5
CHUNK = 8
FACE = 4
ADVANCE = 4
SCALE = 2.0 ** 60
LEGS = ((0, 1), (2, 3), (4,))

A0, A1, A2 = -30.0 / 12.0, 16.0 / 12.0, -1.0 / 12.0
B1, B2 = 8.0 / 12.0, -1.0 / 12.0
DIRECTIONS = ((-1, 0), (1, 0), (0, -1), (0, 1), (-1, -1), (1, -1), (-1, 1), (1, 1))
MESH = pl.DeviceIdType.MESH


def first(plus1, minus1, plus2, minus2):
    return (plus2 - minus2) + (B1 / B2) * (plus1 - minus1)


def city_kernel(
    d_hbm, p_hbm, sh_hbm, bk_hbm, cell_ref, kind_ref, t_hbm, f_hbm,
    f_ref, o_ref,
    raw, t_ref, force, sbuf, buf, sh_ref, bk_ref, ps, pr, gx, ht, th, hx, e_ref, s_ref, q_ref,
    vs, g_all, surf, hot, hotx, lhs, mot, fold,
    load_sem, give_send, give_recv, x_send, x_recv, y_send, y_recv,
    near_send, near_recv, hop_send, hop_recv, surf_send, surf_recv, back_send, back_recv,
):
    f32, bf16 = jnp.float32, jnp.bfloat16
    steps = COUPLINGS * EVERY
    cx, cy = sh_hbm.shape[1], sh_hbm.shape[2]
    nz = sh_hbm.shape[0]
    nr = nz // 2
    half = cy // 2
    rows = 2 * cx
    lo, hi = cx, cx + rows
    arch, width = t_hbm.shape[0], t_hbm.shape[1]
    count = kind_ref.shape[0]
    slab, gy = lax.axis_index("slab"), lax.axis_index("gy")
    slabs, gys = lax.axis_size("slab"), lax.axis_size("gy")
    pairs, pieces = slabs // 2, 2 * gys
    k, a = lax.div(slab, 2), lax.rem(slab, 2)
    hsel = lax.rem(a + gy, 2)
    piece = 2 * gy + hsel
    yb, cb = lax.div(gy, 2), lax.rem(gy, 2)
    chunks = nr // CHUNK
    groups = arch // UNIT
    units = groups * COUPLINGS

    def exists(dx, dy):
        x, y = k + dx, piece + dy
        return (x >= 0) & (x < pairs) & (y >= 0) & (y < pieces)

    def target(dx, dy):
        if dy == 0:
            return (2 * (k + dx) + a, gy)
        inner = (hsel == 0) if dy > 0 else (hsel == 1)
        return (2 * (k + dx) + jnp.where(inner, 1 - a, a), jnp.where(inner, gy, gy + dy))

    mate = (2 * k + 1 - a, gy)

    def load(i, src, dst):
        return pltpu.make_async_copy(src, dst, load_sem.at[i])

    loads = [
        load(0, d_hbm, raw.at[0:3]),
        load(1, p_hbm, raw.at[3:6]),
        load(2, sh_hbm, raw.at[6]),
        load(3, bk_hbm, raw.at[7]),
        load(4, t_hbm, t_ref),
        load(5, f_hbm, force),
    ]
    for one in loads:
        one.start()

    zero_tile = jnp.zeros((2, 3, nr + 4, cx, cy), f32)
    buf[:, :, :, 0:lo, :] = zero_tile
    buf[:, :, :, hi : hi + cx, :] = zero_tile
    pr[...] = jnp.zeros_like(pr)
    vs[...] = jnp.zeros_like(vs)
    g_rows = 2 * 3
    mot[...] = jnp.zeros_like(mot)

    barrier = pltpu.get_barrier_semaphore()

    def greet(device):
        pl.semaphore_signal(barrier, inc=1, device_id=device, device_id_type=MESH)

    def row_mates():
        for da in range(2):
            for dg in range(gys):
                if da or dg:
                    yield da, dg, (2 * k + lax.rem(a + da, 2), lax.rem(gy + dg, gys))

    for _, _, device in row_mates():
        greet(device)
    for dk in range(1, pairs):
        greet((2 * lax.rem(k + dk, pairs) + a, gy))
    for dx, dy in DIRECTIONS[4:]:
        @pl.when(exists(dx, dy))
        def _():
            greet(target(dx, dy))
    beside = [
        jnp.where(at > 0, 1, 0) + jnp.where(at < size - 1, 1, 0)
        for at, size in ((k, pairs), (piece, pieces))
    ]

    lane = lax.broadcasted_iota(jnp.int32, (cx, cy), 1)
    row = lax.broadcasted_iota(jnp.int32, (cx, cy), 0)
    left = lane < half

    def folded(near, far, second_half):
        if second_half:
            return jnp.where(left, pltpu.roll(near, half, 1), far)
        return jnp.where(left, near, pltpu.roll(far, half, 1))

    own = pl.ds(pl.multiple_of(cx * a, cx), cx)
    own_buf = pl.ds(pl.multiple_of(lo + cx * a, cx), cx)

    def kept_ref(i, r):
        if i < 3:
            return buf.at[0, i, r + 2, own_buf, :]
        if i < 6:
            return buf.at[1, i - 3, r + 2, own_buf, :]
        return (sh_ref if i == 6 else bk_ref).at[r, own, :]

    def give(i):
        if i < 3:
            dst = buf.at[0, i, 2 : nr + 2, own_buf, :]
        elif i < 6:
            dst = buf.at[1, i - 3, 2 : nr + 2, own_buf, :]
        else:
            dst = (sh_ref if i == 6 else bk_ref).at[:, own, :]
        return pltpu.make_async_remote_copy(
            src_ref=sbuf.at[i], dst_ref=dst, send_sem=give_send.at[i], recv_sem=give_recv.at[i],
            device_id=mate, device_id_type=MESH,
        )

    for i in range(8):
        if i in (0, 3, 6, 7):
            loads[{0: 0, 3: 1, 6: 2, 7: 3}[i]].wait()
        for r in range(nr):
            near, far = raw[i, r], raw[i, nz - 1 - r]
            if i >= 6:
                near, far = near * A2, far * A2
            lower, upper = folded(near, far, False), folded(near, far, True)
            kept_ref(i, r)[...] = jnp.where(hsel == 0, lower, upper)
            sbuf[i, r] = jnp.where(hsel == 0, upper, lower)
        if i == 0:
            corners = beside[0] * beside[1]
            pl.semaphore_wait(barrier, pieces - 1 + pairs - 1 + corners)
        give(i).start()

    ny = gys * cy
    cell = cell_ref[...]
    start = slab * cx
    along_x = jnp.zeros_like(cell)
    for i in range(1, cx):
        along_x = along_x + jnp.where(cell >= (start + i) * ny, 1, 0)
    column = cell - (start + along_x) * ny
    hotx[...] = jnp.where(
        lax.broadcasted_iota(jnp.int32, (cx, count), 0) == along_x, 1.0, 0.0
    )
    for i in range(ny // 128):
        hot[128 * i : 128 * (i + 1), :] = jnp.where(
            lax.broadcasted_iota(jnp.int32, (128, count), 0) + 128 * i == column, 1.0, 0.0
        ).astype(bf16)

    loads[4].wait()
    loads[5].wait()

    def face(dx, par, piece_r):
        mine = lo if dx < 0 else hi - 2
        theirs = hi if dx < 0 else lo - 2
        j = 0 if dx < 0 else 1
        span = pl.ds(2 + FACE * piece_r, FACE)
        return pltpu.make_async_remote_copy(
            src_ref=buf.at[par, :, span, mine : mine + 2, :],
            dst_ref=buf.at[par, :, span, theirs : theirs + 2, :],
            send_sem=x_send.at[par, j, piece_r], recv_sem=x_recv.at[par, j, piece_r],
            device_id=target(dx, 0), device_id_type=MESH,
        )

    def edge(j, par, piece_r):
        dx, dy = DIRECTIONS[j]
        side = 1 if dy < 0 else 0
        if dx == 0:
            src = ps.at[par, piece_r]
            dst = pr.at[par, piece_r, side, :, lo:hi, :]
        else:
            mine = 0 if dx < 0 else rows - 2
            theirs = hi if dx < 0 else lo - 2
            src = ps.at[par, piece_r, :, mine : mine + 2, :]
            dst = pr.at[par, piece_r, side, :, theirs : theirs + 2, :]
        return pltpu.make_async_remote_copy(
            src_ref=src, dst_ref=dst, send_sem=y_send.at[par, piece_r, j], recv_sem=y_recv.at[par, piece_r, j],
            device_id=target(dx, dy), device_id_type=MESH,
        )

    def send_face(par, piece_r):
        for dx in (-1, 1):
            @pl.when(exists(dx, 0))
            def _():
                face(dx, par, piece_r).start()

    lane2 = lax.broadcasted_iota(jnp.int32, (rows, cy), 1)
    lanem = lax.rem(lane2, half)

    def send_edges(par, piece_r):
        for c in range(3):
            packed = jnp.zeros((rows, cy), f32)
            for r in range(CHUNK * piece_r, CHUNK * (piece_r + 1)):
                turned = pltpu.roll(buf[par, c, r + 2, lo:hi, :], 2 + 4 * r, 1)
                packed = jnp.where((lanem >= 4 * r) & (lanem < 4 * r + 4), turned, packed)
            ps[par, piece_r, c] = packed
        for j in range(2, 8):
            @pl.when(exists(*DIRECTIONS[j]))
            def _():
                edge(j, par, piece_r).start()

    def wait_halos(par, piece_r):
        for j, dx in enumerate((-1, 1)):
            parts = range(piece_r * CHUNK // FACE, (piece_r + 1) * CHUNK // FACE)
            @pl.when(exists(dx, 0))
            def _():
                for part in parts:
                    face(dx, par, part).wait_send()
            @pl.when(exists(-dx, 0))
            def _():
                for part in parts:
                    face(dx, par, part).wait_recv()
        for j in range(2, 8):
            dx, dy = DIRECTIONS[j]
            @pl.when(exists(dx, dy))
            def _():
                edge(j, par, piece_r).wait_send()
            @pl.when(exists(-dx, -dy))
            def _():
                edge(j, par, piece_r).wait_recv()

    left2 = lane2 < half
    sign = jnp.where(left2, 1.0, -1.0)
    sign1 = jnp.where(left, 1.0, -1.0)
    lm3 = lanem[None]
    lm1 = lax.rem(lane, half)[None]

    def depth_first(plus1, minus1, plus2, minus2, sgn):
        return sgn * ((plus2 - minus2) + (B1 / B2) * (plus1 - minus1))

    def along_y(core, halo, lm):
        return (
            pltpu.roll(jnp.where(lm < 1, halo, core), cy - 1, 2),
            pltpu.roll(jnp.where(lm >= half - 1, halo, core), 1, 2),
            pltpu.roll(jnp.where(lm < 2, halo, core), cy - 2, 2),
            pltpu.roll(jnp.where(lm >= half - 2, halo, core), 2, 2),
        )

    def ghosts(ref, index, span, top):
        at = lambda r: index + (r + 2, span, slice(None))
        if top:
            mask = lax.broadcasted_iota(jnp.int32, (span.stop - span.start, cy), 1) < half
            ref[at(-1)] = jnp.where(mask, ref[at(1)], 0.0)
            ref[at(-2)] = jnp.where(mask, ref[at(2)], 0.0)
        else:
            ref[at(nr)] = pltpu.roll(ref[at(nr - 1)], half, 1)
            ref[at(nr + 1)] = pltpu.roll(ref[at(nr - 2)], half, 1)

    from_left = lax.rem(lane2, 4) < 2
    spot = lax.div(lanem, 4)
    turn = lambda v, by: pltpu.roll(v, by % cy, 1)
    h0_here = (~left2 & from_left) | (left2 & ~from_left)

    def grid_step(n, par):
        new = 1 - par

        def received(c, at, size, piece_r):
            return jnp.where(
                from_left[0:size], pr[par, piece_r, 0, c, at : at + size, :],
                pr[par, piece_r, 1, c, at : at + size, :],
            )

        def joined(c, at, size, last_piece):
            got = received(c, at, size, 0)
            for piece_r in range(1, last_piece + 1):
                got = jnp.where(spot[0:size] < CHUNK * piece_r, got, received(c, at, size, piece_r))
            return got

        def unpack(piece_r, r0, r1, t0, t1):
            g = [joined(c, lo, rows, piece_r) for c in range(3)]
            gx[lo:hi, :] = g[0]
            gx[0:lo, :] = joined(0, 0, cx, piece_r)
            gx[hi : hi + cx, :] = joined(0, hi, cx, piece_r)
            g_y = jnp.where(row < 4, joined(1, hi, cx, piece_r), joined(1, 0, cx, piece_r))
            a_g = first(
                gx[lo + 1 : hi + 1, :], gx[lo - 1 : hi - 1, :],
                gx[lo + 2 : hi + 2, :], gx[lo - 2 : hi - 2, :],
            )
            g2 = g[2]
            plus1, plus2, minus1, minus2 = turn(g2, -4), turn(g2, -8), turn(g2, 4), turn(g2, 8)
            if t0 == 0:
                minus1 = jnp.where(spot == 0, jnp.where(h0_here, turn(g2, -4), 0.0), minus1)
                minus2 = jnp.where(
                    spot == 0, jnp.where(h0_here, turn(g2, -8), 0.0),
                    jnp.where(spot == 1, jnp.where(h0_here, g2, 0.0), minus2),
                )
            if t1 == nr:
                plus1 = jnp.where(spot == nr - 1, turn(g2, half), plus1)
                plus2 = jnp.where(
                    spot < nr - 2, plus2,
                    jnp.where(spot == nr - 2, turn(g2, -(half + 4)), turn(g2, -(half - 4))),
                )
            t_g = a_g + depth_first(plus1, minus1, plus2, minus2, jnp.where(h0_here, 1.0, -1.0))
            for r in range(r0, r1):
                back = (half - 2 - 4 * r) % cy
                for c in range(3):
                    ht[c, r] = turn(g[c], back)
                hx[r] = turn(g_y, back)
            for r in range(t0, t1):
                th[r] = turn(t_g, (half - 2 - 4 * r) % cy)

        def reader(planes):
            def u(c, r, shift, at, size=rows):
                return buf[par, c, pl.ds(r + 2 + shift, planes), at : at + size, :]
            return u

        def prepare(r, planes):
            u = reader(planes)
            x = first(u(0, r, 0, lo + 1), u(0, r, 0, lo - 1), u(0, r, 0, lo + 2), u(0, r, 0, lo - 2))
            y = first(*along_y(u(1, r, 0, lo), ht[1, pl.ds(r, planes)], lm3))
            z = depth_first(u(2, r, 1, lo), u(2, r, -1, lo), u(2, r, 2, lo), u(2, r, -2, lo), sign)
            e_ref[pl.ds(r + 2, planes)] = x + y
            s_ref[pl.ds(r, planes), lo:hi, :] = y + z
            q_ref[pl.ds(r, planes)] = x + z

            def mixed(comp, shift):
                return jnp.where(row[None] < 4, u(comp, r, shift, hi, cx), u(comp, r, shift, 0, cx))

            s_halo = first(*along_y(mixed(1, 0), hx[pl.ds(r, planes)], lm1)) + depth_first(
                mixed(2, 1), mixed(2, -1), mixed(2, 2), mixed(2, -2), sign1
            )
            s_ref[pl.ds(r, planes), 0:lo, :] = s_halo
            s_ref[pl.ds(r, planes), hi : hi + cx, :] = s_halo

        def advance(b, carry):
            u, planes = reader(ADVANCE), ADVANCE
            r = b * ADVANCE
            sh = sh_ref[pl.ds(r, planes)]
            bk = bk_ref[pl.ds(r, planes)]

            def s(at):
                return s_ref[pl.ds(r, planes), at : at + rows, :]

            def e(shift):
                return e_ref[pl.ds(r + 2 + shift, planes)]

            for c in range(3):
                mid = u(c, r, 0, lo)
                y = along_y(mid, ht[c, pl.ds(r, planes)], lm3)
                near = [u(c, r, 0, lo + 1) + u(c, r, 0, lo - 1), y[0] + y[1], u(c, r, 1, lo) + u(c, r, -1, lo)]
                far = [u(c, r, 0, lo + 2) + u(c, r, 0, lo - 2), y[2] + y[3], u(c, r, 2, lo) + u(c, r, -2, lo)]
                lap = (3.0 * A0 / A2) * mid + (A1 / A2) * (near[0] + near[1] + near[2]) + (far[0] + far[1] + far[2])
                own_second = (A0 / A2) * mid + (A1 / A2) * near[c] + far[c]
                if c == 0:
                    cross = first(s(lo + 1), s(lo - 1), s(lo + 2), s(lo - 2))
                elif c == 1:
                    cross = first(*along_y(q_ref[pl.ds(r, planes)], th[pl.ds(r, planes)], lm3))
                else:
                    cross = depth_first(e(1), e(-1), e(2), e(-2), sign)
                acc = sh * lap + bk * (own_second + (B2 * B2 / A2) * cross)
                place = (new, c, pl.ds(r + 2, planes), slice(lo, hi), slice(None))
                buf[place] = 2.0 * mid - buf[place] + acc
            return carry

        def share(stop):
            @pl.when(n < steps - 1)
            def _():
                send_face(new, stop // FACE - 1)
                if stop % CHUNK == 0:
                    send_edges(new, stop // CHUNK - 1)

        done, ready, known = 0, 0, 0
        for piece_r in range(chunks):
            wait_halos(par, piece_r)
            last_piece = piece_r == chunks - 1
            if piece_r == 0:
                for c, span in ((0, slice(lo, hi)), (1, slice(lo, hi)), (2, slice(0, hi + cx))):
                    ghosts(buf, (par, c), span, True)
            if last_piece:
                for c, span in ((0, slice(lo, hi)), (1, slice(lo, hi)), (2, slice(0, hi + cx))):
                    ghosts(buf, (par, c), span, False)
            upto = CHUNK * (piece_r + 1)
            safe = nr if last_piece else upto - 2
            unpack(piece_r, known, upto, ready, safe)
            prepare(ready, safe - ready)
            if piece_r == 0:
                ghosts(e_ref, (), slice(0, rows), True)
            if last_piece:
                ghosts(e_ref, (), slice(0, rows), False)
            known, ready = upto, safe
            limit = nr if last_piece else ADVANCE * ((safe - 2) // ADVANCE)
            while done < limit:
                stop = done + FACE
                lax.fori_loop(done // ADVANCE, stop // ADVANCE, advance, 0)
                share(stop)
                if stop == FACE:
                    @pl.when(lax.rem(n, EVERY) == EVERY - 1)
                    def _():
                        send_surface(lax.div(n, EVERY), new)
                done = stop

    def surface_copy(moment, par, da, dg):
        to_a, to_g = lax.rem(a + da, 2), lax.rem(gy + dg, gys)
        at = pl.ds(pl.multiple_of(lo + cx * to_a, cx), cx)
        return pltpu.make_async_remote_copy(
            src_ref=buf.at[par, :, 2, at, :], dst_ref=surf.at[moment, piece],
            send_sem=surf_send.at[moment, gys * da + dg], recv_sem=surf_recv.at[moment, gys * da + dg],
            device_id=(2 * k + to_a, to_g), device_id_type=MESH,
        )

    def send_surface(moment, par):
        for da, dg, _ in row_mates():
            surface_copy(moment, par, da, dg).start()
        surf[moment, piece] = buf[par, :, 2, own_buf, :]

    def gather_motion(moment, par):
        for da, dg, _ in row_mates():
            surface_copy(moment, par, da, dg).wait()
        for j in range(gys):
            for c in range(3):
                even, odd = surf[moment, 2 * j, c], surf[moment, 2 * j + 1, c]
                table = jnp.where(left, even, pltpu.roll(odd, half, 1))
                for part in range(3):
                    piece_of = table.astype(bf16)
                    at = 24 * part + 8 * c
                    lhs[at : at + 8, 128 * j : 128 * (j + 1)] = piece_of.astype(f32)
                    table = table - piece_of.astype(f32)
        found = jnp.dot(lhs[...].astype(bf16), hot[...], preferred_element_type=f32)
        for c in range(3):
            value = found[8 * c : 8 * c + 8] + found[24 + 8 * c : 32 + 8 * c]
            value = value + found[48 + 8 * c : 56 + 8 * c]
            value = jnp.sum(value * hotx[...], axis=0, keepdims=True) * SCALE
            mot[moment, 2 * c : 2 * c + 1, :] = value
            mot[moment, 2 * c + 1 : 2 * c + 2, :] = value

    def unit_span(unit):
        return pl.ds(pl.multiple_of(lax.div(unit, COUPLINGS) * UNIT, UNIT), UNIT), COUPLINGS - 1 - lax.rem(unit, COUPLINGS)

    def g_copy(ref, device, send_sem, recv_sem):
        return pltpu.make_async_remote_copy(
            src_ref=ref, dst_ref=ref, send_sem=send_sem, recv_sem=recv_sem,
            device_id=device, device_id_type=MESH,
        )

    def spread(unit, dk):
        span, moment = unit_span(unit)
        ref = g_all.at[k, a, yb, cb, span, moment, 0:g_rows, :]
        return g_copy(
            ref, (2 * lax.rem(k + dk, pairs) + a, gy), near_send.at[unit, dk - 1], near_recv.at[unit, dk - 1]
        )

    y_mate = (slab, 2 * (1 - yb) + cb)
    c_mate = (slab, 2 * yb + 1 - cb)

    def hop(unit, leg):
        span, moment = unit_span(unit)
        phase, even = divmod(leg, 2)
        if phase < 2:
            span = pl.ds(span.start + (0 if even == 0 else UNIT // 2), UNIT // 2)
        tail = (span, moment, slice(0, g_rows), slice(None))
        every = slice(None)
        if phase == 0:
            ref, device = g_all.at[(every, a, yb, cb) + tail], (mate, y_mate)[even]
        elif phase == 1:
            ref = g_all.at[((every, every, yb, cb) if even == 0 else (every, a, every, cb)) + tail]
            device = (y_mate, mate)[even]
        else:
            ref, device = g_all.at[(every, every, every, cb) + tail], c_mate
        return g_copy(ref, device, hop_send.at[unit, leg], hop_recv.at[unit, leg])

    def respond(unit):
        stage = lax.rem(unit, COUPLINGS)
        group = lax.div(unit, COUPLINGS)

        @pl.when(stage == 0)
        def _():
            span = pl.ds(pl.multiple_of(group * UNIT, UNIT), UNIT)
            rows_of = [force[c, span, :] for c in range(3)]
            for i in range(UNIT):
                for c in range(3):
                    vs[i, c : c + 1, :] = rows_of[c][i : i + 1] * (1.0 / SCALE)

        v = [vs[i] for i in range(UNIT)]
        total = list(v)
        for it in range(SUB):
            for i in range(UNIT):
                high = v[i].astype(bf16)
                low = (v[i] - high.astype(f32)).astype(bf16)
                both = jnp.concatenate([high, low], axis=0)
                got = lax.dot_general(
                    both, t_ref[group * UNIT + i], (((1,), (1,)), ((), ())), preferred_element_type=f32
                )
                v[i] = got[0:8] + got[8:16]
                if it < SUB - 1:
                    total[i] = total[i] + v[i]
        for i in range(UNIT):
            result = jnp.where(stage == 0, total[i], v[i])
            vs[i] = result
            for c in range(3):
                for h in range(2):
                    g_all[k, a, yb, cb, group * UNIT + i, COUPLINGS - 1 - stage, 2 * c + h : 2 * c + h + 1, :] = (
                        result[c : c + 1, 128 * h : 128 * (h + 1)]
                    )

    def tick_links(i):
        for phase in range(5):
            unit = i - 1 - 2 * phase

            @pl.when((unit >= 0) & (unit < units))
            def _():
                if phase == 1:
                    for dk in range(1, pairs):
                        spread(unit, dk).wait_recv()
                elif phase > 1:
                    for leg in LEGS[phase - 2]:
                        hop(unit, leg).wait_recv()
                if phase == 0:
                    for dk in range(1, pairs):
                        spread(unit, dk).start()
                elif phase < 4:
                    for leg in LEGS[phase - 1]:
                        hop(unit, leg).start()

    def body(i, carry):
        n = i - EARLY
        par = lax.rem(n + 2 * EARLY, 2)

        @pl.when(n == 0)
        def _():
            for j in range(8):
                give(j).wait()
            for part in range(nr // FACE):
                send_face(0, part)
            for piece_r in range(chunks):
                send_edges(0, piece_r)

        @pl.when(n >= 0)
        def _():
            grid_step(n, par)

        @pl.when(i < units)
        def _():
            respond(i)

        tick_links(i)

        @pl.when((n > 0) & (lax.rem(n + EARLY * EVERY, EVERY) == EVERY - 1) & (n < steps - 1))
        def _():
            gather_motion(lax.div(n, EVERY), 1 - par)
        return carry

    lax.fori_loop(0, EARLY + steps, body, 0)

    last = steps % 2
    theirs = pl.ds(pl.multiple_of(lo + cx * (1 - a), cx), cx)
    back = pltpu.make_async_remote_copy(
        src_ref=buf.at[last, :, 2 : nr + 2, theirs, :], dst_ref=fold,
        send_sem=back_send.at[0], recv_sem=back_recv.at[0], device_id=mate, device_id_type=MESH,
    )
    back.start()
    gather_motion(COUPLINGS - 1, last)

    for unit in range(units):
        for dk in range(1, pairs):
            spread(unit, dk).wait_send()
        for leg in range(5):
            hop(unit, leg).wait_send()

    table = g_all.reshape(slabs * gys * arch, COUPLINGS, 8, 128)
    row8 = lax.broadcasted_iota(jnp.int32, (8, 128), 0)

    def tile(j, carry):
        lanes = pl.ds(pl.multiple_of(128 * j, 128), 128)
        motion = [mot[m, :, lanes] for m in range(COUPLINGS)]

        for i in range(16):
            base = pl.multiple_of(128 * j + 8 * i, 8)
            out = [jnp.zeros((8, 128), f32)] * 2
            for b in range(8):
                kind = kind_ref[128 * j + 8 * i + b]
                got = None
                for m in range(COUPLINGS):
                    at = 8 * i + b
                    term = jnp.broadcast_to(motion[m][:, at : at + 1], (8, 128)) * table[kind, m]
                    got = term if got is None else got + term
                got = jnp.where(row8 < g_rows, got, 0.0)
                got = got + pltpu.roll(got, 4, 0)
                got = got + pltpu.roll(got, 2, 0)
                moved = pltpu.roll(got, 1, 0)
                here, there = (got, moved) if b % 2 == 0 else (moved, got)
                out = [jnp.where(row8 == b, one, so_far) for one, so_far in zip((here, there), out)]
            o_ref[pl.ds(base, 8), 0:128] = out[0]
            o_ref[pl.ds(base, 8), 128:256] = out[1]
        return carry

    lax.fori_loop(0, count // 128, tile, 0)

    back.wait()
    for c in range(3):
        for r in range(nr):
            mine, other = buf[last, c, r + 2, own_buf, :], fold[c, r]
            lower = jnp.where(hsel == 0, mine, other)
            upper = jnp.where(hsel == 0, other, mine)
            f_ref[c, r] = jnp.where(left, lower, pltpu.roll(upper, half, 1))
            f_ref[c, nz - 1 - r] = jnp.where(left, pltpu.roll(lower, half, 1), upper)


def per_device(
    displacement, previous, shear_coef, bulk_coef, cell_index, archetype_id, transition, forcing
):
    _, nz, cx, cy = displacement.shape
    arch, width, _ = transition.shape
    count = cell_index.shape[0]
    slabs, gys = lax.axis_size("slab"), lax.axis_size("gy")
    pairs, nr, rows = slabs // 2, nz // 2, 2 * cx
    tall = rows + 2 * cx
    units = arch // UNIT * COUPLINGS
    chunks = nr // CHUNK
    f32 = jnp.float32
    vmem, dma = pltpu.VMEM, pltpu.SemaphoreType.DMA
    whole = pl.BlockSpec(memory_space=pltpu.VMEM)
    away = pl.BlockSpec(memory_space=pl.ANY)
    return pl.pallas_call(
        city_kernel,
        out_shape=(
            jax.ShapeDtypeStruct(displacement.shape, f32),
            jax.ShapeDtypeStruct((count, width), f32),
        ),
        in_specs=[away] * 4 + [whole, pl.BlockSpec(memory_space=pltpu.SMEM), away, away],
        out_specs=(whole, whole),
        scratch_shapes=[
            vmem((8, nz, cx, cy), f32),
            vmem((arch, width, width), jnp.bfloat16),
            vmem((3, arch, width), f32),
            vmem((8, nr, cx, cy), f32),
            vmem((2, 3, nr + 4, tall, cy), f32),
            vmem((nr, rows, cy), f32),
            vmem((nr, rows, cy), f32),
            vmem((2, chunks, 3, rows, cy), f32),
            vmem((2, chunks, 2, 3, tall, cy), f32),
            vmem((tall, cy), f32),
            vmem((3, nr, rows, cy), f32),
            vmem((nr, rows, cy), f32),
            vmem((nr, cx, cy), f32),
            vmem((nr + 4, rows, cy), f32),
            vmem((nr, tall, cy), f32),
            vmem((nr, rows, cy), f32),
            vmem((UNIT, 8, width), f32),
            vmem((pairs, 2, 2, gys // 2, arch, COUPLINGS, 8, 128), f32),
            vmem((COUPLINGS, 2 * gys, 3, cx, cy), f32),
            vmem((gys * cy, count), jnp.bfloat16),
            vmem((cx, count), f32),
            vmem((72, gys * cy), f32),
            vmem((COUPLINGS, 8, count), f32),
            vmem((3, nr, cx, cy), f32),
            dma((6,)),
            dma((8,)),
            dma((8,)),
            dma((2, 2, nr // FACE)),
            dma((2, 2, nr // FACE)),
            dma((2, chunks, 8)),
            dma((2, chunks, 8)),
            dma((units, pairs - 1)),
            dma((units, pairs - 1)),
            dma((units, 5)),
            dma((units, 5)),
            dma((COUPLINGS, 2 * gys)),
            dma((COUPLINGS, 2 * gys)),
            dma((1,)),
            dma((1,)),
        ],
        compiler_params=pltpu.CompilerParams(
            collective_id=0, has_side_effects=True, vmem_limit_bytes=60 * 1024 * 1024
        ),
    )(
        displacement, previous, shear_coef, bulk_coef, cell_index.reshape(1, count),
        archetype_id[:, 0], transition, forcing.transpose(1, 0, 2),
    )


def solution(mesh):
    in_specs = (
        P(None, None, "slab", "gy"),
        P(None, None, "slab", "gy"),
        P(None, "slab", "gy"),
        P(None, "slab", "gy"),
        P(("slab", "gy")),
        P(("slab", "gy"), None),
        P(("slab", "gy"), None, None),
        P(("slab", "gy"), None, None),
    )
    out_specs = (P(None, None, "slab", "gy"), P(("slab", "gy"), None))
    return jax.shard_map(
        per_device, mesh=mesh, in_specs=in_specs, out_specs=out_specs, check_vma=False
    )
```
